256 devices in a mesh: member: 64 (over y, z, core), region: 4 (over x).
Axes of the slice: x: 4, y: 4, z: 8, core: 2. Of those that a mesh axis runs over, the one named last changes fastest.
Arguments:
- ensemble: bfloat16 [512, 262144], P(('member', 'region')), may hold values from -12 to 12
- obs_offset: int32 [4, 64, 16], P('region', 'member'), may hold values from 0 to 1023
- observed: float32 [4, 64, 16], P('region', 'member'), may hold values from -12 to 12
- obs_var: float32 [4, 64, 16], P('region', 'member'), may hold values from 0.2 to 2
Outputs:
- analysis: bfloat16 [512, 262144], P(('member', 'region'))
The draws below stay inside these ranges and needn't reach their ends.
Inputs may be any that keep to these rules, and one draw needn't show every extreme that they name: obs_offset indexes a link within the block of 1024 links; two detectors may watch the same link.
All inputs are finite; a program needn't handle non-finite values.
Results may differ from the reference program's by a relative error of at most 0.0019.
Values may be sent and summed in bfloat16 or wider, within the bound.
A program may use at most 128 MiB of HBM per device.

```python
import math
import jax
import jax.numpy as jnp
from jax import lax

M = 512
LINK_DEV = 1024
OBS_DEV = 16
REGION_LINKS = 65536
S = 262144
N_MEMBER = 64
N_REGION = 4


def draw_ensemble(key, part):
    values = jax.random.normal(key, (M, S), jnp.float32)
    return jnp.clip(values, -6.0, 6.0).astype(jnp.bfloat16)


def place_ends(entries, stream_key, smallest, top_value):
    place = [jax.random.randint(jax.random.fold_in(stream_key, axis), (), 0, length) for axis, length in enumerate(entries.shape)]
    widest = entries.shape.index(max(entries.shape))
    beside = place[:widest] + [(place[widest] + 1) % entries.shape[widest]] + place[widest + 1:]
    return entries.at[tuple(place)].set(smallest).at[tuple(beside)].set(top_value)


def block_levels(key, shape, shards, low, high):
    loudness = 1.0
    for axis_at, parts in shards:
        steps = jax.random.uniform(jax.random.fold_in(jax.random.fold_in(key, 6), axis_at), (parts,), jnp.float32, low / len(shards), high / len(shards))
        loudness = loudness * jnp.repeat(jnp.exp(steps), shape[axis_at] // parts).reshape((-1,) + (1,) * (len(shape) - 1 - axis_at))
    return loudness


def scatter_about(rng, shape, scale, bound, pieces=(), kind=jnp.bfloat16):
    level = block_levels(rng, shape, pieces, -0.22, 0.18) if pieces else 1.0
    entries = jax.random.normal(rng, shape, jnp.float32) * scale * level
    return jnp.minimum(jnp.maximum(entries, -bound), bound).astype(kind)


def setup_inputs(seed: int = 0) -> dict:
    streams_of = jax.random.split(jax.random.key(seed), 5)
    return {
        "ensemble": draw_ensemble(jax.random.fold_in(streams_of[4], 71), 0),
        "obs_offset": place_ends(jax.random.randint(streams_of[1], (N_REGION, N_MEMBER, OBS_DEV), 0, LINK_DEV), jax.random.fold_in(streams_of[1], 1), 0, LINK_DEV - 1).astype(jnp.int32),
        "observed": scatter_about(streams_of[2], (N_REGION, N_MEMBER, OBS_DEV), 2.0, 12.0, ((0, 4), (1, 64)), jnp.float32),
        "obs_var": jnp.clip(jnp.exp(math.log(2.0) - 2.3025851 * jax.random.uniform(streams_of[3], (N_REGION, N_MEMBER, OBS_DEV), jnp.float32) ** block_levels(streams_of[3], (N_REGION, N_MEMBER, OBS_DEV), ((0, 4), (1, 64)), -0.2, 0.2)), 0.2, 2.0),
    }


def observation_terms(picked, values, variance, ensemble_size):
    center = lax.optimization_barrier(jnp.mean(picked, axis=1, keepdims=True))
    anomaly = picked - center
    innovation = values - center[:, 0]
    numer = jnp.sum(innovation * innovation)
    denom = jnp.sum(lax.optimization_barrier(jnp.sum(anomaly * anomaly, axis=1)) / (ensemble_size - 1.0) + variance)
    weight = 1.0 / ((ensemble_size - 1.0) * variance)
    return (anomaly, innovation, weight, numer, denom)

def weighted_products(anomaly, innovation, weight):
    weighted = anomaly * weight[:, None]
    products = jnp.dot(weighted.T, anomaly, precision=lax.Precision.HIGHEST)
    column = jnp.dot(innovation * weight, anomaly, precision=lax.Precision.HIGHEST)
    return (products, column)

def mixing_matrix(products, column, lift, diag_coef, col_coef, mat_coef):
    identity = jnp.eye(products.shape[0], dtype=jnp.float32)
    system = identity + lift * products
    factor = jnp.linalg.cholesky(system)
    right_side = jnp.concatenate([products, column[:, None]], axis=1)
    solved = jax.scipy.linalg.cho_solve((factor, True), right_side)
    return diag_coef * identity + col_coef * solved[:, -1][None, :] - mat_coef * solved[:, :-1]

def reference(ensemble, obs_offset, observed, obs_var):
    ensemble_size = ensemble.shape[0]
    link_total = ensemble.shape[1]
    region_idx = lax.broadcasted_iota(jnp.int32, obs_offset.shape, 0)
    member_idx = lax.broadcasted_iota(jnp.int32, obs_offset.shape, 1)
    link_index = (region_idx * REGION_LINKS + member_idx * LINK_DEV + obs_offset.astype(jnp.int32)).reshape(-1).astype(jnp.int32)
    picked = jnp.take(ensemble, link_index, axis=1).T.astype(jnp.float32)
    anomaly, innovation, weight, numer, denom = observation_terms(picked, observed.reshape(-1), obs_var.reshape(-1), ensemble_size)
    products, column = weighted_products(anomaly, innovation, weight)
    inflation = jnp.sqrt(numer / denom)
    mixing = mixing_matrix(products, column, inflation * inflation, inflation, inflation * inflation, 0.5 * inflation * inflation * inflation)

    def update_block(block):
        state_values = block.astype(jnp.float32)
        center = lax.optimization_barrier(jnp.mean(state_values, axis=0, keepdims=True))
        return (center + jnp.dot(mixing, state_values - center, precision=lax.Precision.HIGHEST)).astype(jnp.bfloat16)
    blocks = jnp.moveaxis(ensemble.reshape(ensemble_size, -1, LINK_DEV), 1, 0)
    updated = lax.map(update_block, blocks)
    return jnp.moveaxis(updated, 0, 1).reshape(ensemble_size, link_total)
```

```python
import jax
import jax.numpy as jnp
from jax import lax
from jax.experimental import pallas as pl
from jax.experimental.pallas import tpu as pltpu
from jax.sharding import Mesh
from jax.sharding import PartitionSpec as P

MEMBER = ("member_0", "member_1", "member_2")
REGION_MEMBER = ("region", "member_0", "member_1", "member_2")
MEMBER_REGION = ("member_0", "member_1", "member_2", "region")


def split_up(x, dim, devices):
    dims = x.shape
    pieces = x.reshape(*dims[:dim], devices, dims[dim] // devices, *dims[dim + 1 :])
    return jnp.moveaxis(pieces, dim, 0)


def laid_out(pieces, dim):
    pieces = jnp.moveaxis(pieces, 0, dim)
    dims = pieces.shape
    return pieces.reshape(*dims[:dim], dims[dim] * dims[dim + 1], *dims[dim + 2 :])


def one_exchange(x, axis, axes, splits, concats):
    sizes = [lax.axis_size(a) for a in axes]
    pieces = split_up(x, splits[0], sizes[0])
    pieces = jnp.moveaxis(split_up(pieces, splits[1] + 1, sizes[1]), 0, 1)
    inside = pieces.shape[2:]
    pieces = pieces.reshape(-1, *inside)
    pieces = lax.all_to_all(pieces, axis, split_axis=0, concat_axis=0, tiled=True)
    pieces = laid_out(pieces.reshape(*sizes, *inside), concats[0] + 1)
    return laid_out(pieces, concats[1])


def sent_and_summed(x, axis, dim):
    devices = lax.axis_size(axis)
    pieces = lax.all_to_all(split_up(x, dim, devices), axis, 0, 0, tiled=True)
    return jnp.sum(pieces, axis=0)


def sum_by_axis(x, axes, dim):
    far, near = axes
    pieces = split_up(x, dim, lax.axis_size(far))
    nearer = sent_and_summed(pieces, near, dim + 1)
    arrived = lax.all_to_all(nearer, far, split_axis=0, concat_axis=0, tiled=True)
    return arrived.sum(axis=0)


def rows_for(lines, devices):
    spare = -len(lines) % devices
    return jnp.pad(lines, [(0, spare)] + [(0, 0)] * (lines.ndim - 1))


def from_everyone(x, axis):
    devices = lax.axis_size(axis)
    return lax.all_to_all(jnp.broadcast_to(x[None], (devices, *x.shape)), axis, 0, 0, tiled=True)


def whole_of(x, axes, dim):
    far, near = axes
    first = from_everyone(x, far)
    pieces = jnp.swapaxes(from_everyone(first, near), 0, 1)
    return laid_out(pieces.reshape(-1, *x.shape), dim)


def sum_by_parts(x, axes):
    own = sum_by_axis(rows_for(x, lax.axis_size(axes[0]) * lax.axis_size(axes[1])), axes, 0)
    whole = whole_of(own, axes, 0)
    return whole[: len(x)].reshape(x.shape)


def together(arrays, axis):
    ends = [0]
    for a in arrays:
        ends.append(ends[-1] + a.size)
    total = sum_by_parts(jnp.concatenate([a.ravel() for a in arrays]), axis)
    return tuple((total[b:e].reshape(a.shape) for a, b, e in zip(arrays, ends, ends[1:])))


def observation_terms(picked, values, variance, ensemble_size):
    center = jnp.mean(picked, axis=1, keepdims=True)
    anomaly = picked - center
    innovation = values - center[:, 0]
    numer = jnp.sum(innovation * innovation)
    denom = jnp.sum(jnp.sum(anomaly * anomaly, axis=1) / (ensemble_size - 1.0) + variance)
    weight = 1.0 / ((ensemble_size - 1.0) * variance)
    return (anomaly, innovation, weight, numer, denom)


def weighted_products(anomaly, innovation, weight):
    weighted = anomaly * weight[:, None]
    products = jnp.dot(weighted.T, anomaly, precision=lax.Precision.HIGHEST)
    column = jnp.dot(innovation * weight, anomaly, precision=lax.Precision.HIGHEST)
    return (products, column)


def split_bf16(a):
    high = a.astype(jnp.bfloat16)
    return high, (a - high.astype(jnp.float32)).astype(jnp.bfloat16)


def dot1(a, b):
    return jnp.dot(
        a.astype(jnp.bfloat16), b.astype(jnp.bfloat16), preferred_element_type=jnp.float32
    )


def dot3(a, b):
    ah, al = split_bf16(a)
    bh, bl = split_bf16(b)
    return dot1(ah, bh) + (dot1(ah, bl) + dot1(al, bh))


def dot6(a, b):
    return jnp.dot(a, b, precision=lax.Precision.HIGHEST, preferred_element_type=jnp.float32)


TILE = 128
WELL_CONDITIONED = 600.0
ROUNDING = 1e-6


def by_rows(rows, body, init=None):
    def step(i, carry):
        return body(pl.ds(pl.multiple_of(i * TILE, TILE), TILE), carry)

    return lax.fori_loop(0, rows // TILE, step, init)


def largest_row(m):
    return jnp.max(jnp.sum(jnp.abs(m), axis=1))


def sum_of_squares(m):
    return jnp.sum(m * m)


def unit(rows, n):
    row = lax.broadcasted_iota(jnp.int32, (TILE, n), 0) + rows.start
    col = lax.broadcasted_iota(jnp.int32, (TILE, n), 1)
    return jnp.where(row == col, 1.0, 0.0).astype(jnp.float32)


def inverse_into(x, system, r, tmp):
    n = system.shape[0]

    def series(dot, enough):
        def square(rows, bound):
            tmp[rows, :] = dot(system[rows, :], system[...])
            return jnp.maximum(bound, largest_row(tmp[rows, :]))

        bound = jnp.sqrt(by_rows(n, square, jnp.float32(0.0)) * 1.02)
        a = 2.0 / (1.0 + bound)

        def first(rows, total):
            eye = unit(rows, n)
            s = system[rows, :] * a
            x[rows, :] = a * (2.0 * eye - s)
            left = eye - 2.0 * s + (a * a) * tmp[rows, :]
            r[rows, :] = left
            return total + sum_of_squares(left)

        size = by_rows(n, first, jnp.float32(0.0))

        def more(state):
            count, size = state
            return jnp.logical_and(count < 40, size > enough * enough)

        def double(state):
            count, _ = state

            def grow(rows, _):
                x[rows, :] += dot(x[rows, :], r[...])
                tmp[rows, :] = dot(r[rows, :], r[...])
                return 0

            by_rows(n, grow, 0)

            def take(rows, total):
                left = tmp[rows, :]
                r[rows, :] = left
                return total + sum_of_squares(left)

            return count + 1, by_rows(n, take, jnp.float32(0.0))

        lax.while_loop(more, double, (jnp.int32(0), size))

    def newton(dot, dot_step):
        def more(state):
            count, size = state
            return jnp.logical_and(count < 12, size > ROUNDING)

        def step(state):
            count, _ = state

            def residual(rows, total):
                left = unit(rows, n) - dot(system[rows, :], x[...])
                r[rows, :] = left
                return total + sum_of_squares(left)

            size = by_rows(n, residual, jnp.float32(0.0))

            def correct(rows, _):
                x[rows, :] += dot_step(x[rows, :], r[...])
                return 0

            by_rows(n, correct, 0)
            return count + 1, size

        return lax.while_loop(more, step, (jnp.int32(0), jnp.float32(1.0)))[1]

    bound = by_rows(n, lambda rows, m: jnp.maximum(m, largest_row(system[rows, :])), jnp.float32(0.0))
    easy = bound < WELL_CONDITIONED

    def quick():
        series(dot1, 0.1)
        return newton(dot3, dot3)

    left = lax.cond(easy, quick, lambda: jnp.float32(1.0))

    @pl.when(jnp.logical_not(left <= ROUNDING))
    def _():
        series(dot6, 0.02)
        newton(dot6, dot6)


def analysis_kernel(products, column, sums, state, out, x, system, r, tmp):
    n = products.shape[0]
    square = sums[0] / sums[1]
    inflation = jnp.sqrt(jnp.full((1, n), square, jnp.float32))

    def scaled(rows, trace):
        eye = unit(rows, n)
        p = products[rows, :] * square
        system[rows, :] = eye + p
        return trace + jnp.sum(eye * p)

    trace = by_rows(n, scaled, jnp.float32(0.0))
    shift = trace / ((n - 1.0) * n)

    def shifted(rows, _):
        system[rows, :] += shift
        return 0

    by_rows(n, shifted, 0)
    inverse_into(x, system, r, tmp)

    q = dot6(column[...], x[...])

    def mix(rows, _):
        eye = unit(rows, n)
        mixing = 0.5 * inflation * (eye + x[rows, :]) + square * q
        mean = jnp.sum(mixing, axis=1, keepdims=True) * (1.0 / n)
        high, low = split_bf16(mixing - mean + 1.0 / n)
        out[rows, :] = (dot1(high, state[...]) + dot1(low, state[...])).astype(jnp.bfloat16)
        return 0

    by_rows(n, mix, 0)


def analysed(products, column, numer, denom, state):
    n = products.shape[0]
    sums = jnp.stack([numer, denom])
    vmem = pl.BlockSpec(memory_space=pltpu.VMEM)
    return pl.pallas_call(
        analysis_kernel,
        name="analysis",
        out_shape=jax.ShapeDtypeStruct(state.shape, jnp.bfloat16),
        in_specs=[vmem, vmem, pl.BlockSpec(memory_space=pltpu.SMEM), vmem],
        out_specs=vmem,
        scratch_shapes=[pltpu.VMEM((n, n), jnp.float32) for _ in range(4)],
    )(products, column[None, :], sums, state)


def local(ensemble, obs_offset, observed, obs_var):
    members = lax.axis_size(MEMBER)
    regions = lax.axis_size("region")
    own_count = ensemble.shape[0]
    ensemble_size = own_count * members * regions
    shifted = one_exchange(ensemble, REGION_MEMBER, ("region", MEMBER), (1, 1), (0, 0))
    offsets = obs_offset.reshape(-1)
    values = observed.reshape(-1)
    variance = obs_var.reshape(-1)
    picked = jnp.take(shifted, offsets, axis=1).T.astype(jnp.float32)
    anomaly, innovation, weight, numer, denom = observation_terms(
        picked, values, variance, ensemble_size
    )
    products, column = weighted_products(anomaly, innovation, weight)
    products, column, numer, denom = together(
        (products, column, numer, denom), (("member_0", "member_1"), ("member_2", "region"))
    )
    updated = analysed(products, column, numer, denom, shifted)
    return one_exchange(updated, MEMBER_REGION, (MEMBER, "region"), (0, 0), (1, 1))


def solution(mesh):
    finer = Mesh(
        mesh.devices.reshape(4, 8, 2, mesh.shape["region"]),
        ("member_0", "member_1", "member_2", "region"),
    )
    in_specs = (
        P(MEMBER_REGION, None),
        P("region", MEMBER, None),
        P("region", MEMBER, None),
        P("region", MEMBER, None),
    )
    out_specs = P(MEMBER_REGION, None)
    return jax.shard_map(local, mesh=finer, in_specs=in_specs, out_specs=out_specs, check_vma=False)
```

```python
import jax
import jax.numpy as jnp
from jax import lax
from jax.experimental import pallas as pl
from jax.experimental.pallas import tpu as pltpu
from jax.sharding import Mesh
from jax.sharding import PartitionSpec as P

MEMBER = ("member_0", "member_1", "member_2")
REGION_MEMBER = ("region", "member_0", "member_1", "member_2")
MEMBER_REGION = ("member_0", "member_1", "member_2", "region")


MESH_ID = pl.DeviceIdType.MESH
SIDE_Y, SIDE_Z, CORES, SIDE_X = 4, 8, 2, 4


def here():
    return (
        lax.axis_index("region"),
        lax.axis_index("member_0"),
        lax.axis_index("member_1"),
        lax.axis_index("member_2"),
    )


def device(x, y, z, c):
    return (y, z, c, x)


def in_plane(i):
    return lax.rem(i // 4, 4), lax.rem(i // 16, 2), lax.rem(i, 4)


PLANE = SIDE_X * SIDE_Y * CORES


def plane_peer(i):
    x, y, z, c = here()
    dy, dc, dx = in_plane(i)
    return lax.rem(x + dx, SIDE_X), lax.rem(y + dy, SIDE_Y), z, lax.rem(c + dc, CORES)


def line_peer(i):
    x, y, z, c = here()
    return x, y, lax.rem(z + i, SIDE_Z), c


def greet(barrier):
    @pl.loop(1, PLANE)
    def _(i):
        pl.semaphore_signal(barrier, 1, device_id=device(*plane_peer(i)), device_id_type=MESH_ID)

    @pl.loop(1, SIDE_Z)
    def _(i):
        pl.semaphore_signal(barrier, 1, device_id=device(*line_peer(i)), device_id_type=MESH_ID)


def met(barrier):
    pl.semaphore_wait(barrier, PLANE - 1 + SIDE_Z - 1)


def remote(src, dst, send, recv, place):
    return pltpu.make_async_remote_copy(
        src, dst, send, recv, device_id=device(*place), device_id_type=MESH_ID
    )


def block_of(x, y, z, c):
    return ((x * SIDE_Y + y) * SIDE_Z + z) * CORES + c


def links_of(block, size):
    return pl.ds(pl.multiple_of(block * size, size), size)


def gather_kernel(own, whole, stage, send_p, recv_p, send_z, recv_z):
    x, y, z, c = here()
    size = whole.shape[-1]
    barrier = pltpu.get_barrier_semaphore()
    greet(barrier)
    met(barrier)

    @pl.loop(1, PLANE)
    def _(i):
        px, py, _, pc = plane_peer(i)

        @pl.loop(0, SIDE_Z)
        def _(t):
            remote(
                own.at[:, links_of(block_of(px, py, t, pc), size)],
                stage.at[t, y, c * SIDE_X + x],
                send_p,
                recv_p,
                (px, py, z, pc),
            ).start()

    @pl.loop(0, SIDE_Z)
    def _(t):
        stage[t, y, c * SIDE_X + x] = own[:, links_of(block_of(x, y, t, c), size)]

    arrived = own.at[:, pl.ds(0, (PLANE - 1) * SIDE_Z * size)]
    remote(arrived, arrived, send_p, recv_p, (x, y, z, c)).wait()

    @pl.loop(1, SIDE_Z)
    def _(i):
        place = line_peer(i)
        remote(stage.at[place[2]], whole.at[:, z], send_z, recv_z, place).start()

    whole[:, z] = stage[z]
    arrived = stage.at[pl.ds(0, SIDE_Z - 1)]
    remote(arrived, arrived, send_z, recv_z, (x, y, z, c)).wait()


def scatter_kernel(whole, own, stage, send_z, recv_z, send_p, recv_p):
    x, y, z, c = here()
    size = whole.shape[-1]
    barrier = pltpu.get_barrier_semaphore()
    greet(barrier)
    met(barrier)

    @pl.loop(1, SIDE_Z)
    def _(i):
        place = line_peer(i)
        remote(whole.at[:, place[2]], stage.at[z], send_z, recv_z.at[z], place).start()

    def hand_on(source, block):
        @pl.loop(1, PLANE)
        def _(j):
            px, py, _, pc = plane_peer(j)
            remote(
                source.at[py, pc * SIDE_X + px],
                own.at[:, links_of(block, size)],
                send_p,
                recv_p,
                (px, py, z, pc),
            ).start()

        own[:, links_of(block, size)] = source[y, c * SIDE_X + x]

    hand_on(whole.at[:, z], block_of(x, y, z, c))

    @pl.loop(1, SIDE_Z)
    def _(i):
        t = lax.rem(z + SIDE_Z - i, SIDE_Z)
        remote(stage.at[t], stage.at[t], send_z, recv_z.at[t], (x, y, z, c)).wait_recv()
        hand_on(stage.at[t], block_of(x, y, t, c))

    arrived = stage.at[pl.ds(0, SIDE_Z - 1)]
    remote(arrived, arrived, send_z, recv_z.at[0], (x, y, z, c)).wait_send()
    arrived = own.at[:, pl.ds(0, (PLANE - 1) * SIDE_Z * size)]
    remote(arrived, arrived, send_p, recv_p, (x, y, z, c)).wait()


VMEM = pl.BlockSpec(memory_space=pltpu.VMEM)


def gathered(own):
    size = own.shape[1] // (PLANE * SIDE_Z)
    return pl.pallas_call(
        gather_kernel,
        name="gather",
        out_shape=jax.ShapeDtypeStruct(
            (SIDE_Y, SIDE_Z, CORES * SIDE_X, own.shape[0], size), own.dtype
        ),
        in_specs=[VMEM],
        out_specs=VMEM,
        scratch_shapes=[
            pltpu.VMEM((SIDE_Z, SIDE_Y, CORES * SIDE_X, own.shape[0], size), own.dtype),
            pltpu.SemaphoreType.DMA,
            pltpu.SemaphoreType.DMA,
            pltpu.SemaphoreType.DMA,
            pltpu.SemaphoreType.DMA,
        ],
        compiler_params=pltpu.CompilerParams(collective_id=0, has_side_effects=True),
    )(own)


def scattered(whole):
    rows, size = whole.shape[-2:]
    return pl.pallas_call(
        scatter_kernel,
        name="scatter",
        out_shape=jax.ShapeDtypeStruct((rows, size * PLANE * SIDE_Z), whole.dtype),
        in_specs=[VMEM],
        out_specs=VMEM,
        scratch_shapes=[
            pltpu.VMEM((SIDE_Z, SIDE_Y, CORES * SIDE_X, rows, size), whole.dtype),
            pltpu.SemaphoreType.DMA,
            pltpu.SemaphoreType.DMA((SIDE_Z,)),
            pltpu.SemaphoreType.DMA,
            pltpu.SemaphoreType.DMA,
        ],
        compiler_params=pltpu.CompilerParams(collective_id=1, has_side_effects=True),
    )(whole)


def split_up(x, dim, devices):
    dims = x.shape
    pieces = x.reshape(*dims[:dim], devices, dims[dim] // devices, *dims[dim + 1 :])
    return jnp.moveaxis(pieces, dim, 0)


def laid_out(pieces, dim):
    pieces = jnp.moveaxis(pieces, 0, dim)
    dims = pieces.shape
    return pieces.reshape(*dims[:dim], dims[dim] * dims[dim + 1], *dims[dim + 2 :])


def sent_and_summed(x, axis, dim):
    devices = lax.axis_size(axis)
    pieces = lax.all_to_all(split_up(x, dim, devices), axis, 0, 0, tiled=True)
    return jnp.sum(pieces, axis=0)


def sum_by_axis(x, axes, dim):
    far, near = axes
    pieces = split_up(x, dim, lax.axis_size(far))
    nearer = sent_and_summed(pieces, near, dim + 1)
    arrived = lax.all_to_all(nearer, far, split_axis=0, concat_axis=0, tiled=True)
    return arrived.sum(axis=0)


def rows_for(lines, devices):
    spare = -len(lines) % devices
    return jnp.pad(lines, [(0, spare)] + [(0, 0)] * (lines.ndim - 1))


def from_everyone(x, axis):
    devices = lax.axis_size(axis)
    return lax.all_to_all(jnp.broadcast_to(x[None], (devices, *x.shape)), axis, 0, 0, tiled=True)


def whole_of(x, axes, dim):
    far, near = axes
    first = from_everyone(x, far)
    pieces = jnp.swapaxes(from_everyone(first, near), 0, 1)
    return laid_out(pieces.reshape(-1, *x.shape), dim)


def sum_by_parts(x, axes):
    own = sum_by_axis(rows_for(x, lax.axis_size(axes[0]) * lax.axis_size(axes[1])), axes, 0)
    whole = whole_of(own, axes, 0)
    return whole[: len(x)].reshape(x.shape)


def together(arrays, axis):
    ends = [0]
    for a in arrays:
        ends.append(ends[-1] + a.size)
    total = sum_by_parts(jnp.concatenate([a.ravel() for a in arrays]), axis)
    return tuple((total[b:e].reshape(a.shape) for a, b, e in zip(arrays, ends, ends[1:])))


def observation_terms(picked, values, variance, ensemble_size):
    center = jnp.mean(picked, axis=1, keepdims=True)
    anomaly = picked - center
    innovation = values - center[:, 0]
    numer = jnp.sum(innovation * innovation)
    denom = jnp.sum(jnp.sum(anomaly * anomaly, axis=1) / (ensemble_size - 1.0) + variance)
    weight = 1.0 / ((ensemble_size - 1.0) * variance)
    return (anomaly, innovation, weight, numer, denom)


def weighted_products(anomaly, innovation, weight):
    weighted = anomaly * weight[:, None]
    products = jnp.dot(weighted.T, anomaly, precision=lax.Precision.HIGHEST)
    column = jnp.dot(innovation * weight, anomaly, precision=lax.Precision.HIGHEST)
    return (products, column)


def split_bf16(a):
    high = a.astype(jnp.bfloat16)
    return high, (a - high.astype(jnp.float32)).astype(jnp.bfloat16)


def dot1(a, b):
    return jnp.dot(
        a.astype(jnp.bfloat16), b.astype(jnp.bfloat16), preferred_element_type=jnp.float32
    )


def dot3(a, b):
    ah, al = split_bf16(a)
    bh, bl = split_bf16(b)
    return dot1(ah, bh) + (dot1(ah, bl) + dot1(al, bh))


def dot6(a, b):
    return jnp.dot(a, b, precision=lax.Precision.HIGHEST, preferred_element_type=jnp.float32)


TILE = 128
WELL_CONDITIONED = 600.0
ROUNDING = 1e-6


def by_rows(rows, body, init=None):
    def step(i, carry):
        return body(pl.ds(pl.multiple_of(i * TILE, TILE), TILE), carry)

    return lax.fori_loop(0, rows // TILE, step, init)


def largest_row(m):
    return jnp.max(jnp.sum(jnp.abs(m), axis=1))


def sum_of_squares(m):
    return jnp.sum(m * m)


def unit(rows, n):
    row = lax.broadcasted_iota(jnp.int32, (TILE, n), 0) + rows.start
    col = lax.broadcasted_iota(jnp.int32, (TILE, n), 1)
    return jnp.where(row == col, 1.0, 0.0).astype(jnp.float32)


def inverse_into(x, system, r, tmp):
    n = system.shape[0]

    def series(dot, enough):
        def square(rows, bound):
            tmp[rows, :] = dot(system[rows, :], system[...])
            return jnp.maximum(bound, largest_row(tmp[rows, :]))

        bound = jnp.sqrt(by_rows(n, square, jnp.float32(0.0)) * 1.02)
        a = 2.0 / (1.0 + bound)

        def first(rows, total):
            eye = unit(rows, n)
            s = system[rows, :] * a
            x[rows, :] = a * (2.0 * eye - s)
            left = eye - 2.0 * s + (a * a) * tmp[rows, :]
            r[rows, :] = left
            return total + sum_of_squares(left)

        size = by_rows(n, first, jnp.float32(0.0))

        def more(state):
            count, size = state
            return jnp.logical_and(count < 40, size > enough * enough)

        def double(state):
            count, _ = state

            def grow(rows, _):
                x[rows, :] += dot(x[rows, :], r[...])
                tmp[rows, :] = dot(r[rows, :], r[...])
                return 0

            by_rows(n, grow, 0)

            def take(rows, total):
                left = tmp[rows, :]
                r[rows, :] = left
                return total + sum_of_squares(left)

            return count + 1, by_rows(n, take, jnp.float32(0.0))

        lax.while_loop(more, double, (jnp.int32(0), size))

    def newton(dot, dot_step):
        def more(state):
            count, size = state
            return jnp.logical_and(count < 12, size > ROUNDING)

        def step(state):
            count, _ = state

            def residual(rows, total):
                left = unit(rows, n) - dot(system[rows, :], x[...])
                r[rows, :] = left
                return total + sum_of_squares(left)

            size = by_rows(n, residual, jnp.float32(0.0))

            def correct(rows, _):
                x[rows, :] += dot_step(x[rows, :], r[...])
                return 0

            by_rows(n, correct, 0)
            return count + 1, size

        return lax.while_loop(more, step, (jnp.int32(0), jnp.float32(1.0)))[1]

    bound = by_rows(n, lambda rows, m: jnp.maximum(m, largest_row(system[rows, :])), jnp.float32(0.0))
    easy = bound < WELL_CONDITIONED

    def quick():
        series(dot1, 0.1)
        return newton(dot3, dot3)

    left = lax.cond(easy, quick, lambda: jnp.float32(1.0))

    @pl.when(jnp.logical_not(left <= ROUNDING))
    def _():
        series(dot6, 0.02)
        newton(dot6, dot6)


def analysis_kernel(products, column, sums, state, out, x, system, r, tmp):
    n = products.shape[0]
    square = sums[0] / sums[1]
    inflation = jnp.sqrt(jnp.full((1, n), square, jnp.float32))

    def scaled(rows, trace):
        eye = unit(rows, n)
        p = products[rows, :] * square
        system[rows, :] = eye + p
        return trace + jnp.sum(eye * p)

    trace = by_rows(n, scaled, jnp.float32(0.0))
    shift = trace / ((n - 1.0) * n)

    def shifted(rows, _):
        system[rows, :] += shift
        return 0

    by_rows(n, shifted, 0)
    inverse_into(x, system, r, tmp)

    q = dot6(column[...], x[...])

    def mix(rows, _):
        eye = unit(rows, n)
        mixing = 0.5 * inflation * (eye + x[rows, :]) + square * q
        mean = jnp.sum(mixing, axis=1, keepdims=True) * (1.0 / n)
        high, low = split_bf16(mixing - mean + 1.0 / n)
        out[rows, :] = (dot1(high, state[...]) + dot1(low, state[...])).astype(jnp.bfloat16)
        return 0

    by_rows(n, mix, 0)


def analysed(products, column, numer, denom, state):
    n = products.shape[0]
    sums = jnp.stack([numer, denom])
    vmem = pl.BlockSpec(memory_space=pltpu.VMEM)
    return pl.pallas_call(
        analysis_kernel,
        name="analysis",
        out_shape=jax.ShapeDtypeStruct(state.shape, jnp.bfloat16),
        in_specs=[vmem, vmem, pl.BlockSpec(memory_space=pltpu.SMEM), vmem],
        out_specs=vmem,
        scratch_shapes=[pltpu.VMEM((n, n), jnp.float32) for _ in range(4)],
    )(products, column[None, :], sums, state)


def local(ensemble, obs_offset, observed, obs_var):
    members = lax.axis_size(MEMBER)
    regions = lax.axis_size("region")
    own_count = ensemble.shape[0]
    ensemble_size = own_count * members * regions
    shifted = gathered(ensemble).reshape(ensemble_size, -1)
    offsets = obs_offset.reshape(-1)
    values = observed.reshape(-1)
    variance = obs_var.reshape(-1)
    picked = jnp.take(shifted, offsets, axis=1).T.astype(jnp.float32)
    anomaly, innovation, weight, numer, denom = observation_terms(
        picked, values, variance, ensemble_size
    )
    products, column = weighted_products(anomaly, innovation, weight)
    products, column, numer, denom = together(
        (products, column, numer, denom), (("member_0", "member_1"), ("member_2", "region"))
    )
    updated = analysed(products, column, numer, denom, shifted)
    return scattered(
        updated.reshape(SIDE_Y, SIDE_Z, CORES * SIDE_X, own_count, updated.shape[1])
    )


def solution(mesh):
    finer = Mesh(
        mesh.devices.reshape(4, 8, 2, mesh.shape["region"]),
        ("member_0", "member_1", "member_2", "region"),
    )
    in_specs = (
        P(MEMBER_REGION, None),
        P("region", MEMBER, None),
        P("region", MEMBER, None),
        P("region", MEMBER, None),
    )
    out_specs = P(MEMBER_REGION, None)
    return jax.shard_map(local, mesh=finer, in_specs=in_specs, out_specs=out_specs, check_vma=False)
```

```python
import jax
import jax.numpy as jnp
from jax import lax
from jax.experimental import pallas as pl
from jax.experimental.pallas import tpu as pltpu
from jax.sharding import Mesh
from jax.sharding import PartitionSpec as P

MEMBER = ("member_0", "member_1", "member_2")
MEMBER_REGION = ("member_0", "member_1", "member_2", "region")


MESH_ID = pl.DeviceIdType.MESH
SIDE_Y, SIDE_Z, CORES, SIDE_X = 4, 8, 2, 4


def here():
    return (
        lax.axis_index("region"),
        lax.axis_index("member_0"),
        lax.axis_index("member_1"),
        lax.axis_index("member_2"),
    )


def device(x, y, z, c):
    return (y, z, c, x)


def chip_peer(i):
    x, y, z, c = here()
    return lax.rem(x + i, SIDE_X), lax.rem(y + i // SIDE_X, SIDE_Y), z, c


def in_plane(i):
    return lax.rem(i // 4, 4), lax.rem(i // 16, 2), lax.rem(i, 4)


PLANE = SIDE_X * SIDE_Y * CORES


def plane_peer(i):
    x, y, z, c = here()
    dy, dc, dx = in_plane(i)
    return lax.rem(x + dx, SIDE_X), lax.rem(y + dy, SIDE_Y), z, lax.rem(c + dc, CORES)


def line_peer(i):
    x, y, z, c = here()
    return x, y, lax.rem(z + i, SIDE_Z), c


def greet(barrier):
    @pl.loop(1, PLANE)
    def _(i):
        pl.semaphore_signal(barrier, 1, device_id=device(*plane_peer(i)), device_id_type=MESH_ID)

    @pl.loop(1, SIDE_Z)
    def _(i):
        pl.semaphore_signal(barrier, 1, device_id=device(*line_peer(i)), device_id_type=MESH_ID)


def met(barrier):
    pl.semaphore_wait(barrier, PLANE - 1 + SIDE_Z - 1)


def remote(src, dst, send, recv, place):
    return pltpu.make_async_remote_copy(
        src, dst, send, recv, device_id=device(*place), device_id_type=MESH_ID
    )


def block_of(x, y, z, c):
    return ((x * SIDE_Y + y) * SIDE_Z + z) * CORES + c


def links_of(block, size):
    return pl.ds(pl.multiple_of(block * size, size), size)


def no_matter(ref, send, recv):
    return remote(ref, ref, send, recv, here())


def dot6_t(a, b):
    return lax.dot_general(
        a,
        b,
        (((1,), (1,)), ((), ())),
        precision=lax.Precision.HIGHEST,
        preferred_element_type=jnp.float32,
    )


def gather_kernel(
    own, notes, whole, total, sums,
    pieces, stage, all_notes, seen, picked, product, half, chunks, extras, other, send, recv,
):
    x, y, z, c = here()
    size = own.shape[1] // (PLANE * SIDE_Z)
    members = total.shape[0]
    seat = c * SIDE_X + x
    barrier = pltpu.get_barrier_semaphore()
    greet(barrier)
    met(barrier)

    @pl.loop(1, SIDE_Z)
    def _(i):
        remote(notes, all_notes.at[z], send.at[0], recv.at[0], line_peer(i)).start()

    @pl.loop(1, PLANE)
    def _(i):
        px, py, _, pc = plane_peer(i)

        @pl.loop(0, SIDE_Z)
        def _(t):
            remote(
                own.at[:, links_of(block_of(px, py, t, pc), size)],
                pieces.at[t, y, seat],
                send.at[1],
                recv.at[1],
                (px, py, z, pc),
            ).start()

    all_notes[z] = notes[...]

    @pl.loop(0, SIDE_Z)
    def _(t):
        pieces[t, y, seat] = own[:, links_of(block_of(x, y, t, c), size)]

    no_matter(all_notes.at[pl.ds(0, SIDE_Z - 1)], send.at[0], recv.at[0]).wait()
    table = jnp.sum(all_notes[...], axis=0)
    offset = table[0:1, :].astype(jnp.int32)
    measured = table[1:2, :]
    variance = table[2:3, :]
    watches = table.shape[1]
    link = lax.broadcasted_iota(jnp.int32, (size, watches), 0)
    seen[...] = jnp.where(link == offset, 1.0, 0.0).astype(jnp.bfloat16)

    no_matter(own.at[:, pl.ds(0, (PLANE - 1) * SIDE_Z * size)], send.at[1], recv.at[1]).wait()
    line = lax.broadcasted_iota(jnp.int32, (members // SIDE_Z, watches), 1) // (watches // SIDE_Z)

    def pick(t, found):
        def lay(k, _):
            stage[t, k] = pieces[t, k].reshape(stage.shape[2:])
            return 0

        lax.fori_loop(0, SIDE_Y, lay, 0)
        rows = stage[t].reshape(members // SIDE_Z, size)
        values = jnp.dot(rows, seen[...], preferred_element_type=jnp.float32)
        return jnp.where(line == t, values, found)

    found = lax.fori_loop(0, SIDE_Z, pick, jnp.zeros(line.shape, jnp.float32))
    mine = picked.at[SIDE_Z]
    mine[...] = found.astype(jnp.bfloat16).reshape(mine.shape)

    @pl.loop(1, SIDE_Z)
    def _(i):
        remote(mine, picked.at[z], send.at[2], recv.at[2], line_peer(i)).start()

    @pl.loop(1, SIDE_Z)
    def _(i):
        place = line_peer(i)
        remote(stage.at[place[2]], whole.at[:, z], send.at[3], recv.at[3], place).start()

    picked[z] = mine[...]
    whole[:, z] = stage[z]
    no_matter(picked.at[pl.ds(0, SIDE_Z - 1)], send.at[2], recv.at[2]).wait()

    values = jnp.swapaxes(picked[pl.ds(0, SIDE_Z)], 0, 1).reshape(members, watches)
    values = values.astype(jnp.float32)
    center = jnp.sum(values, axis=0, keepdims=True) * (1.0 / members)
    anomaly = values - center
    innovation = measured - center
    weight = 1.0 / ((members - 1.0) * variance)
    spread = jnp.sum(anomaly * anomaly, axis=0, keepdims=True) * (1.0 / (members - 1.0)) + variance
    column = dot6_t(weight * innovation, anomaly)
    numer = jnp.sum(innovation * innovation, axis=1, keepdims=True)
    denom = jnp.sum(spread, axis=1, keepdims=True)
    lane = lax.broadcasted_iota(jnp.int32, column.shape, 1)
    extra = extras.at[PLANE]
    extra[0:1, :] = column
    extra[1:2, :] = jnp.where(lane == 0, numer, jnp.where(lane == 1, denom, 0.0))
    product[...] = dot6_t(anomaly * weight, anomaly)

    rows = members // CORES
    kept = pl.ds(pl.multiple_of(c * rows, rows), rows)
    given = pl.ds(pl.multiple_of((1 - c) * rows, rows), rows)
    partner = (x, y, z, 1 - c)
    remote(product.at[given], other, send.at[4], recv.at[4], partner).start()

    @pl.loop(1, PLANE)
    def _(i):
        remote(
            extra, extras.at[y * (CORES * SIDE_X) + seat], send.at[5], recv.at[5], plane_peer(i)
        ).start()

    extras[y * (CORES * SIDE_X) + seat] = extra[...]
    no_matter(other, send.at[4], recv.at[4]).wait()
    half[...] = product[kept, :] + other[...]
    chips = SIDE_X * SIDE_Y
    part = rows // chips

    def part_of(px, py, base=0):
        return pl.ds(pl.multiple_of(base + (py * SIDE_X + px) * part, part), part)

    @pl.loop(1, chips)
    def _(i):
        place = chip_peer(i)
        remote(
            half.at[part_of(place[0], place[1])],
            chunks.at[y * SIDE_X + x],
            send.at[6],
            recv.at[6],
            place,
        ).start()

    chunks[y * SIDE_X + x] = half[part_of(x, y), :]
    no_matter(chunks.at[pl.ds(0, chips - 1)], send.at[6], recv.at[6]).wait()
    done = total.at[part_of(x, y, c * rows)]
    done[...] = jnp.sum(chunks[...], axis=0)

    @pl.loop(1, chips)
    def _(i):
        remote(done, done, send.at[7], recv.at[7], chip_peer(i)).start()

    no_matter(half.at[pl.ds(0, rows - part)], send.at[7], recv.at[7]).wait()
    remote(total.at[kept], total.at[kept], send.at[8], recv.at[8], partner).start()
    no_matter(extras.at[pl.ds(0, PLANE - 1)], send.at[5], recv.at[5]).wait()
    sums[...] = jnp.sum(extras[pl.ds(0, PLANE)], axis=0)
    no_matter(other, send.at[8], recv.at[8]).wait()
    no_matter(stage.at[pl.ds(0, SIDE_Z - 1)], send.at[3], recv.at[3]).wait()


def scatter_kernel(high, low, state, own, whole, stage, send_z, recv_z, send_p, recv_p):
    x, y, z, c = here()
    rows, size = state.shape
    barrier = pltpu.get_barrier_semaphore()
    greet(barrier)
    wide = 256

    @pl.loop(0, size // wide)
    def _(k):
        at = links_of(k, wide)
        values = dot1(high[...], state[:, at]) + dot1(low[...], state[:, at])
        whole[:, :, :, :, at] = values.astype(jnp.bfloat16).reshape(*whole.shape[:-1], wide)

    met(barrier)

    @pl.loop(1, SIDE_Z)
    def _(i):
        place = line_peer(i)
        remote(whole.at[:, place[2]], stage.at[z], send_z, recv_z.at[z], place).start()

    def hand_on(source, block):
        @pl.loop(1, PLANE)
        def _(j):
            px, py, _, pc = plane_peer(j)
            remote(
                source.at[py, pc * SIDE_X + px],
                own.at[:, links_of(block, size)],
                send_p,
                recv_p,
                (px, py, z, pc),
            ).start()

        own[:, links_of(block, size)] = source[y, c * SIDE_X + x]

    hand_on(whole.at[:, z], block_of(x, y, z, c))

    @pl.loop(1, SIDE_Z)
    def _(i):
        t = lax.rem(z + SIDE_Z - i, SIDE_Z)
        remote(stage.at[t], stage.at[t], send_z, recv_z.at[t], (x, y, z, c)).wait_recv()
        hand_on(stage.at[t], block_of(x, y, t, c))

    arrived = stage.at[pl.ds(0, SIDE_Z - 1)]
    remote(arrived, arrived, send_z, recv_z.at[0], (x, y, z, c)).wait_send()
    arrived = own.at[:, pl.ds(0, (PLANE - 1) * SIDE_Z * size)]
    remote(arrived, arrived, send_p, recv_p, (x, y, z, c)).wait()


VMEM = pl.BlockSpec(memory_space=pltpu.VMEM)


def gathered(own, notes, members):
    size = own.shape[1] // (PLANE * SIDE_Z)
    seats = CORES * SIDE_X
    rows = own.shape[0]
    watches = notes.shape[1]
    part = (members // CORES) // (SIDE_X * SIDE_Y)
    f32, bf16 = jnp.float32, jnp.bfloat16
    return pl.pallas_call(
        gather_kernel,
        name="gather",
        out_shape=(
            jax.ShapeDtypeStruct((SIDE_Y, SIDE_Z, seats * rows, size), bf16),
            jax.ShapeDtypeStruct((members, members), f32),
            jax.ShapeDtypeStruct((2, members), f32),
        ),
        in_specs=[VMEM, VMEM],
        out_specs=(VMEM, VMEM, VMEM),
        scratch_shapes=[
            pltpu.VMEM((SIDE_Z, SIDE_Y, seats, rows, size), bf16),
            pltpu.VMEM((SIDE_Z, SIDE_Y, seats * rows, size), bf16),
            pltpu.VMEM((SIDE_Z, *notes.shape), f32),
            pltpu.VMEM((size, watches), bf16),
            pltpu.VMEM((SIDE_Z + 1, SIDE_Y, seats * rows, watches), bf16),
            pltpu.VMEM((members, members), f32),
            pltpu.VMEM((members // CORES, members), f32),
            pltpu.VMEM((SIDE_X * SIDE_Y, part, members), f32),
            pltpu.VMEM((PLANE + 1, 2, members), f32),
            pltpu.VMEM((members // CORES, members), f32),
            pltpu.SemaphoreType.DMA((9,)),
            pltpu.SemaphoreType.DMA((9,)),
        ],
        compiler_params=pltpu.CompilerParams(collective_id=0, has_side_effects=True),
    )(own, notes)


def scattered(high, low, state, own_rows):
    rows, size = state.shape
    shape = (SIDE_Y, SIDE_Z, CORES * SIDE_X, own_rows, size)
    return pl.pallas_call(
        scatter_kernel,
        name="scatter",
        out_shape=jax.ShapeDtypeStruct((own_rows, size * PLANE * SIDE_Z), state.dtype),
        in_specs=[VMEM, VMEM, VMEM],
        out_specs=VMEM,
        scratch_shapes=[
            pltpu.VMEM(shape, state.dtype),
            pltpu.VMEM((SIDE_Z, SIDE_Y, *shape[2:]), state.dtype),
            pltpu.SemaphoreType.DMA,
            pltpu.SemaphoreType.DMA((SIDE_Z,)),
            pltpu.SemaphoreType.DMA,
            pltpu.SemaphoreType.DMA,
        ],
        compiler_params=pltpu.CompilerParams(collective_id=1, has_side_effects=True),
    )(high, low, state)


def split_bf16(a):
    high = a.astype(jnp.bfloat16)
    return high, (a - high.astype(jnp.float32)).astype(jnp.bfloat16)


def dot1(a, b):
    return jnp.dot(
        a.astype(jnp.bfloat16), b.astype(jnp.bfloat16), preferred_element_type=jnp.float32
    )


def dot3(a, b):
    ah, al = split_bf16(a)
    bh, bl = split_bf16(b)
    return dot1(ah, bh) + (dot1(ah, bl) + dot1(al, bh))


def dot6(a, b):
    return jnp.dot(a, b, precision=lax.Precision.HIGHEST, preferred_element_type=jnp.float32)


TILE = 128
WELL_CONDITIONED = 600.0
ROUNDING = 1e-6


def by_rows(rows, body, init=None):
    def step(i, carry):
        return body(pl.ds(pl.multiple_of(i * TILE, TILE), TILE), carry)

    return lax.fori_loop(0, rows // TILE, step, init)


def largest_row(m):
    return jnp.max(jnp.sum(jnp.abs(m), axis=1))


def sum_of_squares(m):
    return jnp.sum(m * m)


def unit(rows, n):
    row = lax.broadcasted_iota(jnp.int32, (TILE, n), 0) + rows.start
    col = lax.broadcasted_iota(jnp.int32, (TILE, n), 1)
    return jnp.where(row == col, 1.0, 0.0).astype(jnp.float32)


def inverse_into(x, system, r, tmp):
    n = system.shape[0]

    def series(dot, enough):
        def square(rows, bound):
            tmp[rows, :] = dot(system[rows, :], system[...])
            return jnp.maximum(bound, largest_row(tmp[rows, :]))

        bound = jnp.sqrt(by_rows(n, square, jnp.float32(0.0)) * 1.02)
        a = 2.0 / (1.0 + bound)

        def first(rows, total):
            eye = unit(rows, n)
            s = system[rows, :] * a
            x[rows, :] = a * (2.0 * eye - s)
            left = eye - 2.0 * s + (a * a) * tmp[rows, :]
            r[rows, :] = left
            return total + sum_of_squares(left)

        size = by_rows(n, first, jnp.float32(0.0))

        def more(state):
            count, size = state
            return jnp.logical_and(count < 40, size > enough * enough)

        def double(state):
            count, _ = state

            def grow(rows, _):
                x[rows, :] += dot(x[rows, :], r[...])
                tmp[rows, :] = dot(r[rows, :], r[...])
                return 0

            by_rows(n, grow, 0)

            def take(rows, total):
                left = tmp[rows, :]
                r[rows, :] = left
                return total + sum_of_squares(left)

            return count + 1, by_rows(n, take, jnp.float32(0.0))

        lax.while_loop(more, double, (jnp.int32(0), size))

    def newton(dot, dot_step):
        def more(state):
            count, size = state
            return jnp.logical_and(count < 12, size > ROUNDING)

        def step(state):
            count, _ = state

            def residual(rows, total):
                left = unit(rows, n) - dot(system[rows, :], x[...])
                r[rows, :] = left
                return total + sum_of_squares(left)

            size = by_rows(n, residual, jnp.float32(0.0))

            def correct(rows, _):
                x[rows, :] += dot_step(x[rows, :], r[...])
                return 0

            by_rows(n, correct, 0)
            return count + 1, size

        return lax.while_loop(more, step, (jnp.int32(0), jnp.float32(1.0)))[1]

    bound = by_rows(n, lambda rows, m: jnp.maximum(m, largest_row(system[rows, :])), jnp.float32(0.0))
    easy = bound < WELL_CONDITIONED

    def quick():
        series(dot1, 0.1)
        return newton(dot3, dot3)

    left = lax.cond(easy, quick, lambda: jnp.float32(1.0))

    @pl.when(jnp.logical_not(left <= ROUNDING))
    def _():
        series(dot6, 0.02)
        newton(dot6, dot6)


def mixing_kernel(products, sums, high, low, x, system, r, tmp):
    n = products.shape[0]
    square = jnp.sum(sums[1:2, 0:1] / sums[1:2, 1:2])
    inflation = jnp.sqrt(jnp.full((1, n), square, jnp.float32))

    def scaled(rows, trace):
        eye = unit(rows, n)
        p = products[rows, :] * square
        system[rows, :] = eye + p
        return trace + jnp.sum(eye * p)

    trace = by_rows(n, scaled, jnp.float32(0.0))
    shift = trace / ((n - 1.0) * n)

    def shifted(rows, _):
        system[rows, :] += shift
        return 0

    by_rows(n, shifted, 0)
    inverse_into(x, system, r, tmp)

    q = dot6(sums[0:1, :], x[...])

    def mix(rows, _):
        eye = unit(rows, n)
        mixing = 0.5 * inflation * (eye + x[rows, :]) + square * q
        mean = jnp.sum(mixing, axis=1, keepdims=True) * (1.0 / n)
        high[rows, :], low[rows, :] = split_bf16(mixing - mean + 1.0 / n)
        return 0

    by_rows(n, mix, 0)


def mixed(products, sums):
    n = products.shape[0]
    return pl.pallas_call(
        mixing_kernel,
        name="mixing",
        out_shape=[jax.ShapeDtypeStruct((n, n), jnp.bfloat16)] * 2,
        in_specs=[VMEM, VMEM],
        out_specs=[VMEM, VMEM],
        scratch_shapes=[pltpu.VMEM((n, n), jnp.float32) for _ in range(4)],
    )(products, sums)


def local(ensemble, obs_offset, observed, obs_var):
    own_rows = ensemble.shape[0]
    members = own_rows * PLANE * SIDE_Z
    count = obs_offset.size
    notes = jnp.concatenate(
        [obs_offset.astype(jnp.float32).reshape(1, -1), observed.reshape(1, -1), obs_var.reshape(1, -1)]
    )
    notes = jnp.pad(notes, ((0, 5), (0, 0)))
    seat = lax.broadcasted_iota(jnp.int32, (8, SIDE_Z * count), 1) // count
    notes = jnp.where(seat == lax.axis_index("member_1"), jnp.tile(notes, (1, SIDE_Z)), 0.0)
    state, products, sums = gathered(ensemble, notes, members)
    high, low = mixed(products, sums)
    return scattered(high, low, state.reshape(members, -1), own_rows)


def solution(mesh):
    finer = Mesh(
        mesh.devices.reshape(4, 8, 2, mesh.shape["region"]),
        ("member_0", "member_1", "member_2", "region"),
    )
    in_specs = (
        P(MEMBER_REGION, None),
        P("region", MEMBER, None),
        P("region", MEMBER, None),
        P("region", MEMBER, None),
    )
    out_specs = P(MEMBER_REGION, None)
    return jax.shard_map(local, mesh=finer, in_specs=in_specs, out_specs=out_specs, check_vma=False)
```

```python
import jax
import jax.numpy as jnp
from jax import lax
from jax.experimental import pallas as pl
from jax.experimental.pallas import tpu as pltpu
from jax.sharding import Mesh
from jax.sharding import PartitionSpec as P

MEMBER = ("member_0", "member_1", "member_2")
MEMBER_REGION = ("member_0", "member_1", "member_2", "region")


MESH_ID = pl.DeviceIdType.MESH
SIDE_Y, SIDE_Z, CORES, SIDE_X = 4, 8, 2, 4


def here():
    return (
        lax.axis_index("region"),
        lax.axis_index("member_0"),
        lax.axis_index("member_1"),
        lax.axis_index("member_2"),
    )


def device(x, y, z, c):
    return (y, z, c, x)


def chip_peer(i):
    x, y, z, c = here()
    return lax.rem(x + i, SIDE_X), lax.rem(y + i // SIDE_X, SIDE_Y), z, c


def in_plane(i):
    return lax.rem(i // 4, 4), lax.rem(i // 16, 2), lax.rem(i, 4)


PLANE = SIDE_X * SIDE_Y * CORES


def plane_peer(i):
    x, y, z, c = here()
    dy, dc, dx = in_plane(i)
    return lax.rem(x + dx, SIDE_X), lax.rem(y + dy, SIDE_Y), z, lax.rem(c + dc, CORES)


def line_peer(i):
    x, y, z, c = here()
    return x, y, lax.rem(z + i, SIDE_Z), c


def greet(barrier):
    @pl.loop(1, PLANE)
    def _(i):
        pl.semaphore_signal(barrier, 1, device_id=device(*plane_peer(i)), device_id_type=MESH_ID)

    @pl.loop(1, SIDE_Z)
    def _(i):
        pl.semaphore_signal(barrier, 1, device_id=device(*line_peer(i)), device_id_type=MESH_ID)


def met(barrier):
    pl.semaphore_wait(barrier, PLANE - 1 + SIDE_Z - 1)


def remote(src, dst, send, recv, place):
    return pltpu.make_async_remote_copy(
        src, dst, send, recv, device_id=device(*place), device_id_type=MESH_ID
    )


def block_of(x, y, z, c):
    return ((x * SIDE_Y + y) * SIDE_Z + z) * CORES + c


def links_of(block, size):
    return pl.ds(pl.multiple_of(block * size, size), size)


def no_matter(ref, send, recv):
    return remote(ref, ref, send, recv, here())


def dot6_t(a, b):
    return lax.dot_general(
        a,
        b,
        (((1,), (1,)), ((), ())),
        precision=lax.Precision.HIGHEST,
        preferred_element_type=jnp.float32,
    )


def along(k):
    d = k // 2 + 1
    return lax.rem(jnp.where(lax.rem(k, 2) == 0, d, SIDE_Z - d), SIDE_Z) * jnp.where(k == 7, 0, 1)


EARLY = 4


def gather_kernel(
    ensemble, offsets, observed, variances, whole, total, sums,
    own, notes, numbers, pieces, stage, all_notes, seen, picked, product, half, chunks, extras,
    other, copied, send, recv, arrived,
):
    x, y, z, c = here()
    size = own.shape[1] // (PLANE * SIDE_Z)
    members = total.shape[0]
    seat = c * SIDE_X + x
    loads = [
        pltpu.make_async_copy(ensemble, own, copied.at[0]),
        pltpu.make_async_copy(offsets.at[0], numbers, copied.at[1]),
        pltpu.make_async_copy(observed.at[0], notes.at[pl.ds(1, 1), :], copied.at[2]),
        pltpu.make_async_copy(variances.at[0], notes.at[pl.ds(2, 1), :], copied.at[3]),
    ]
    for load in loads:
        load.start()
    barrier = pltpu.get_barrier_semaphore()
    greet(barrier)
    for load in loads:
        load.wait()
    notes[0:1, :] = numbers[...].astype(jnp.float32)
    count, watches = notes.shape[1], all_notes.shape[2]
    to = lax.broadcasted_iota(jnp.int32, (count, watches), 1)
    at = lax.broadcasted_iota(jnp.int32, (count, watches), 0) + z * count
    row = lax.broadcasted_iota(jnp.int32, (8, count), 0)
    placed = dot6(
        jnp.where(row < 3, notes[...], 0.0), jnp.where(to == at, 1.0, 0.0).astype(jnp.float32)
    )
    mine = all_notes.at[SIDE_Z]
    mine[...] = placed

    @pl.loop(0, SIDE_Z)
    def _(t):
        pieces[t, y, seat] = own[:, links_of(block_of(x, y, t, c), size)]

    met(barrier)

    @pl.loop(1, SIDE_Z)
    def _(i):
        remote(mine, all_notes.at[z], send.at[0], recv.at[0], line_peer(i)).start()

    @pl.loop(0, SIDE_Z)
    def _(k):
        t = lax.rem(z + along(k), SIDE_Z)

        @pl.loop(1, PLANE)
        def _(i):
            px, py, _, pc = plane_peer(i)
            remote(
                own.at[:, links_of(block_of(px, py, t, pc), size)],
                pieces.at[t, y, seat],
                send.at[1],
                arrived.at[t],
                (px, py, z, pc),
            ).start()

    all_notes[z] = placed
    no_matter(all_notes.at[pl.ds(0, SIDE_Z - 1)], send.at[0], recv.at[0]).wait()
    table = jnp.sum(all_notes[pl.ds(0, SIDE_Z)], axis=0)
    offset = table[0:1, :].astype(jnp.int32)
    measured = table[1:2, :]
    variance = table[2:3, :]
    link = lax.broadcasted_iota(jnp.int32, (size, watches), 0)
    seen[...] = jnp.where(link == offset, 1.0, 0.0).astype(jnp.bfloat16)
    line = lax.broadcasted_iota(jnp.int32, (members // SIDE_Z, watches), 1) // count

    def pass_on(k):
        t = lax.rem(z + along(k), SIDE_Z)
        remote(stage.at[t], whole.at[:, z], send.at[3], recv.at[3], (x, y, t, c)).start()

    def pick(k, found):
        t = lax.rem(z + along(k), SIDE_Z)
        no_matter(
            own.at[:, pl.ds(0, (PLANE - 1) * size)], send.at[1], arrived.at[t]
        ).wait_recv()

        def lay(j, _):
            stage[t, j] = pieces[t, j].reshape(stage.shape[2:])
            return 0

        lax.fori_loop(0, SIDE_Y, lay, 0)
        rows = stage[t].reshape(members // SIDE_Z, size)
        values = jnp.dot(rows, seen[...], preferred_element_type=jnp.float32)

        @pl.when(jnp.logical_and(k >= 1, k <= EARLY))
        def _():
            pass_on(k - 1)

        return jnp.where(line == t, values, found)

    found = lax.fori_loop(0, SIDE_Z, pick, jnp.zeros(line.shape, jnp.float32))
    mine = picked.at[SIDE_Z]
    mine[...] = found.astype(jnp.bfloat16).reshape(mine.shape)

    @pl.loop(1, SIDE_Z)
    def _(i):
        remote(mine, picked.at[z], send.at[2], recv.at[2], line_peer(i)).start()

    @pl.loop(EARLY, SIDE_Z - 1)
    def _(k):
        pass_on(k)

    picked[z] = mine[...]
    whole[:, z] = stage[z]
    no_matter(
        own.at[:, pl.ds(0, (PLANE - 1) * SIDE_Z * size)], send.at[1], recv.at[1]
    ).wait_send()
    no_matter(picked.at[pl.ds(0, SIDE_Z - 1)], send.at[2], recv.at[2]).wait()

    values = jnp.swapaxes(picked[pl.ds(0, SIDE_Z)], 0, 1).reshape(members, watches)
    values = values.astype(jnp.float32)
    center = jnp.sum(values, axis=0, keepdims=True) * (1.0 / members)
    anomaly = values - center
    innovation = measured - center
    weight = 1.0 / ((members - 1.0) * variance)
    spread = jnp.sum(anomaly * anomaly, axis=0, keepdims=True) * (1.0 / (members - 1.0)) + variance
    column = dot6_t(weight * innovation, anomaly)
    numer = jnp.sum(innovation * innovation, axis=1, keepdims=True)
    denom = jnp.sum(spread, axis=1, keepdims=True)
    lane = lax.broadcasted_iota(jnp.int32, column.shape, 1)
    extra = extras.at[PLANE]
    extra[0:1, :] = column
    extra[1:2, :] = jnp.where(lane == 0, numer, jnp.where(lane == 1, denom, 0.0))
    product[...] = dot6_t(anomaly * weight, anomaly)

    rows = members // CORES
    kept = pl.ds(pl.multiple_of(c * rows, rows), rows)
    given = pl.ds(pl.multiple_of((1 - c) * rows, rows), rows)
    partner = (x, y, z, 1 - c)
    remote(product.at[given], other, send.at[4], recv.at[4], partner).start()

    @pl.loop(1, PLANE)
    def _(i):
        remote(
            extra, extras.at[y * (CORES * SIDE_X) + seat], send.at[5], recv.at[5], plane_peer(i)
        ).start()

    extras[y * (CORES * SIDE_X) + seat] = extra[...]
    no_matter(other, send.at[4], recv.at[4]).wait()
    half[...] = product[kept, :] + other[...]
    chips = SIDE_X * SIDE_Y
    part = rows // chips

    def part_of(px, py, base=0):
        return pl.ds(pl.multiple_of(base + (py * SIDE_X + px) * part, part), part)

    @pl.loop(1, chips)
    def _(i):
        place = chip_peer(i)
        remote(
            half.at[part_of(place[0], place[1])],
            chunks.at[y * SIDE_X + x],
            send.at[6],
            recv.at[6],
            place,
        ).start()

    chunks[y * SIDE_X + x] = half[part_of(x, y), :]
    no_matter(chunks.at[pl.ds(0, chips - 1)], send.at[6], recv.at[6]).wait()
    done = total.at[part_of(x, y, c * rows)]
    done[...] = jnp.sum(chunks[...], axis=0)

    @pl.loop(1, chips)
    def _(i):
        remote(done, done, send.at[7], recv.at[7], chip_peer(i)).start()

    no_matter(half.at[pl.ds(0, rows - part)], send.at[7], recv.at[7]).wait()
    remote(total.at[kept], total.at[kept], send.at[8], recv.at[8], partner).start()
    no_matter(extras.at[pl.ds(0, PLANE - 1)], send.at[5], recv.at[5]).wait()
    sums[...] = jnp.sum(extras[pl.ds(0, PLANE)], axis=0)
    no_matter(other, send.at[8], recv.at[8]).wait()
    no_matter(stage.at[pl.ds(0, SIDE_Z - 1)], send.at[3], recv.at[3]).wait()


def scatter_kernel(high, low, state, own, whole, stage, send_z, recv_z, send_p, recv_p):
    x, y, z, c = here()
    rows, size = state.shape
    barrier = pltpu.get_barrier_semaphore()
    greet(barrier)
    wide = 256

    @pl.loop(0, size // wide)
    def _(k):
        at = links_of(k, wide)
        values = dot1(high[...], state[:, at]) + dot1(low[...], state[:, at])
        whole[:, :, :, :, at] = values.astype(jnp.bfloat16).reshape(*whole.shape[:-1], wide)

    met(barrier)

    @pl.loop(0, SIDE_Z - 1)
    def _(k):
        t = lax.rem(z + along(k), SIDE_Z)

        @pl.loop(0, SIDE_Y)
        def _(dy):
            py = lax.rem(y + dy, SIDE_Y)
            remote(
                whole.at[py, t], stage.at[z, py], send_z, recv_z.at[z, py], (x, y, t, c)
            ).start()

    def hand_on(source, py, dy, block):
        @pl.loop(jnp.where(dy == 0, 1, 0), CORES * SIDE_X)
        def _(j):
            px = lax.rem(x + lax.rem(j, SIDE_X), SIDE_X)
            pc = lax.rem(c + j // SIDE_X, CORES)
            remote(
                source.at[pc * SIDE_X + px],
                own.at[:, links_of(block, size)],
                send_p,
                recv_p,
                (px, py, z, pc),
            ).start()

        @pl.when(dy == 0)
        def _():
            own[:, links_of(block, size)] = source[c * SIDE_X + x]

    @pl.loop(0, SIDE_Y)
    def _(dy):
        py = lax.rem(y + dy, SIDE_Y)
        hand_on(whole.at[py, z], py, dy, block_of(x, y, z, c))

    @pl.loop(0, SIDE_Z - 1)
    def _(k):
        t = lax.rem(z + SIDE_Z - along(k), SIDE_Z)

        @pl.loop(0, SIDE_Y)
        def _(dy):
            py = lax.rem(y + dy, SIDE_Y)
            no_matter(stage.at[t, py], send_z, recv_z.at[t, py]).wait_recv()
            hand_on(stage.at[t, py], py, dy, block_of(x, y, t, c))

    no_matter(stage.at[pl.ds(0, SIDE_Z - 1)], send_z, recv_z.at[0, 0]).wait_send()
    no_matter(own.at[:, pl.ds(0, (PLANE - 1) * SIDE_Z * size)], send_p, recv_p).wait()


VMEM = pl.BlockSpec(memory_space=pltpu.VMEM)


def gathered(own, offsets, observed, variances):
    rows = own.shape[0]
    size = own.shape[1] // (PLANE * SIDE_Z)
    members = rows * PLANE * SIDE_Z
    seats = CORES * SIDE_X
    count = offsets.shape[-1]
    watches = SIDE_Z * count
    part = (members // CORES) // (SIDE_X * SIDE_Y)
    f32, bf16 = jnp.float32, jnp.bfloat16
    return pl.pallas_call(
        gather_kernel,
        name="gather",
        out_shape=(
            jax.ShapeDtypeStruct((SIDE_Y, SIDE_Z, seats * rows, size), bf16),
            jax.ShapeDtypeStruct((members, members), f32),
            jax.ShapeDtypeStruct((2, members), f32),
        ),
        in_specs=[pl.BlockSpec(memory_space=pl.ANY)] * 4,
        out_specs=(VMEM, VMEM, VMEM),
        scratch_shapes=[
            pltpu.VMEM(own.shape, bf16),
            pltpu.VMEM((8, count), f32),
            pltpu.VMEM((1, count), jnp.int32),
            pltpu.VMEM((SIDE_Z, SIDE_Y, seats, rows, size), bf16),
            pltpu.VMEM((SIDE_Z, SIDE_Y, seats * rows, size), bf16),
            pltpu.VMEM((SIDE_Z + 1, 8, watches), f32),
            pltpu.VMEM((size, watches), bf16),
            pltpu.VMEM((SIDE_Z + 1, SIDE_Y, seats * rows, watches), bf16),
            pltpu.VMEM((members, members), f32),
            pltpu.VMEM((members // CORES, members), f32),
            pltpu.VMEM((SIDE_X * SIDE_Y, part, members), f32),
            pltpu.VMEM((PLANE + 1, 2, members), f32),
            pltpu.VMEM((members // CORES, members), f32),
            pltpu.SemaphoreType.DMA((4,)),
            pltpu.SemaphoreType.DMA((9,)),
            pltpu.SemaphoreType.DMA((9,)),
            pltpu.SemaphoreType.DMA((SIDE_Z,)),
        ],
        compiler_params=pltpu.CompilerParams(collective_id=0, has_side_effects=True),
    )(own, offsets, observed, variances)


def scattered(high, low, state, own_rows):
    rows, size = state.shape
    shape = (SIDE_Y, SIDE_Z, CORES * SIDE_X, own_rows, size)
    return pl.pallas_call(
        scatter_kernel,
        name="scatter",
        out_shape=jax.ShapeDtypeStruct((own_rows, size * PLANE * SIDE_Z), state.dtype),
        in_specs=[VMEM, VMEM, VMEM],
        out_specs=VMEM,
        scratch_shapes=[
            pltpu.VMEM(shape, state.dtype),
            pltpu.VMEM((SIDE_Z, SIDE_Y, *shape[2:]), state.dtype),
            pltpu.SemaphoreType.DMA,
            pltpu.SemaphoreType.DMA((SIDE_Z, SIDE_Y)),
            pltpu.SemaphoreType.DMA,
            pltpu.SemaphoreType.DMA,
        ],
        compiler_params=pltpu.CompilerParams(collective_id=1, has_side_effects=True),
    )(high, low, state)


def split_bf16(a):
    high = a.astype(jnp.bfloat16)
    return high, (a - high.astype(jnp.float32)).astype(jnp.bfloat16)


def dot1(a, b):
    return jnp.dot(
        a.astype(jnp.bfloat16), b.astype(jnp.bfloat16), preferred_element_type=jnp.float32
    )


def dot6(a, b):
    return jnp.dot(a, b, precision=lax.Precision.HIGHEST, preferred_element_type=jnp.float32)


TILE = 128
WELL_CONDITIONED = 2000.0
ROUNDING = 1e-6


def by_rows(rows, body, init=None):
    def step(i, carry):
        return body(pl.ds(pl.multiple_of(i * TILE, TILE), TILE), carry)

    return lax.fori_loop(0, rows // TILE, step, init)


def largest_row(m):
    return jnp.max(jnp.sum(jnp.abs(m), axis=1))


def sum_of_squares(m):
    return jnp.sum(m * m)


def unit(rows, n, first=0):
    row = lax.broadcasted_iota(jnp.int32, (TILE, n), 0) + (rows.start - first)
    col = lax.broadcasted_iota(jnp.int32, (TILE, n), 1)
    return jnp.where(row == col, 1.0, 0.0).astype(jnp.float32)


EXTRA = 16


def residual_squares(left):
    return jnp.sum(jnp.sum(left * left, axis=0, keepdims=True))


def quick_inverse(x, system, r, parts, both):
    n = system.shape[1]
    rows = system.shape[0]

    def passes(lhs, rhs):
        return jnp.dot(lhs, rhs, preferred_element_type=jnp.float32)

    values = system[...]
    high = values.astype(jnp.bfloat16)
    parts[pl.ds(0, rows), :] = high
    parts[pl.ds(rows, rows), :] = (values - high.astype(jnp.float32)).astype(jnp.bfloat16)
    top = pl.ds(0, n)
    r[...] = passes(parts[top, :], parts[top, :])
    bound = jnp.sqrt(jnp.max(jnp.sum(jnp.abs(r[...]), axis=0, keepdims=True)) * 1.02)
    a = 2.0 / (1.0 + bound)

    def first(rows, total):
        eye = unit(rows, n)
        s = system[rows, :] * a
        left = eye - 2.0 * s + (a * a) * r[rows, :]
        grown = a * (2.0 * eye - s)
        x[rows, :] = grown
        both[rows, :] = grown.astype(jnp.bfloat16)
        both[pl.ds(n + rows.start, TILE), :] = left.astype(jnp.bfloat16)
        return total + jnp.sum(left * left, axis=0, keepdims=True)

    total = by_rows(n, first, jnp.zeros((1, n), jnp.float32))

    def more(state):
        count, size = state
        return jnp.logical_and(count < 16, size > 0.01)

    def double(state):
        count, _ = state
        out = passes(both[...], both[pl.ds(n, n), :])
        grown = x[top, :] + out[:n]
        left = out[n:]
        x[top, :] = grown
        both[...] = jnp.concatenate([grown, left]).astype(jnp.bfloat16)
        return count + 1, residual_squares(left)

    lax.while_loop(more, double, (jnp.int32(0), jnp.sum(total)))

    def more_newton(state):
        count, size = state
        return jnp.logical_and(count < 8, size > ROUNDING)

    def newton(state):
        count, _ = state
        now = x[top, :]
        xh = now.astype(jnp.bfloat16)
        xl = (now - xh.astype(jnp.float32)).astype(jnp.bfloat16)
        here_high = parts[pl.ds(0, rows), :]
        out = passes(here_high, xh) + (
            passes(here_high, xl) + passes(parts[pl.ds(rows, rows), :], xh)
        )
        r[...] = out[:n]

        def left_of(at, total):
            left = unit(at, n) - r[at, :]
            both[at, :] = left.astype(jnp.bfloat16)
            return total + jnp.sum(left * left, axis=0, keepdims=True)

        total = by_rows(n, left_of, jnp.zeros((1, n), jnp.float32))
        tail = out[n:]
        grown = jnp.concatenate([now, tail])
        x[...] = grown + passes(jnp.concatenate([xh, tail.astype(jnp.bfloat16)]), both[top, :])
        return count + 1, jnp.sum(total)

    return lax.while_loop(more_newton, newton, (jnp.int32(0), jnp.float32(1.0)))[1]


def careful_inverse(x, system, r, tmp):
    n = system.shape[1]

    def square(rows, bound):
        tmp[rows, :] = dot6(system[rows, :], system[pl.ds(0, n), :])
        return jnp.maximum(bound, largest_row(tmp[rows, :]))

    bound = jnp.sqrt(by_rows(n, square, jnp.float32(0.0)) * 1.02)
    a = 2.0 / (1.0 + bound)

    def first(rows, total):
        eye = unit(rows, n)
        s = system[rows, :] * a
        x[rows, :] = a * (2.0 * eye - s)
        left = eye - 2.0 * s + (a * a) * tmp[rows, :]
        r[rows, :] = left
        return total + sum_of_squares(left)

    def more(state):
        count, size = state
        return jnp.logical_and(count < 40, size > 4e-4)

    def double(state):
        def grow(rows, _):
            x[rows, :] += dot6(x[rows, :], r[...])
            tmp[rows, :] = dot6(r[rows, :], r[...])
            return 0

        by_rows(n, grow, 0)

        def take(rows, total):
            left = tmp[rows, :]
            r[rows, :] = left
            return total + sum_of_squares(left)

        return state[0] + 1, by_rows(n, take, jnp.float32(0.0))

    lax.while_loop(more, double, (jnp.int32(0), by_rows(n, first, jnp.float32(0.0))))

    def more_newton(state):
        count, size = state
        return jnp.logical_and(count < 12, size > ROUNDING)

    def newton(state):
        def residual(rows, total):
            left = unit(rows, n) - dot6(system[rows, :], x[pl.ds(0, n), :])
            r[rows, :] = left
            return total + sum_of_squares(left)

        size = by_rows(n, residual, jnp.float32(0.0))

        def correct(rows, _):
            x[rows, :] += dot6(x[rows, :], r[...])
            return 0

        by_rows(n, correct, 0)
        return state[0] + 1, size

    lax.while_loop(more_newton, newton, (jnp.int32(0), jnp.float32(1.0)))
    last = pl.ds(n, system.shape[0] - n)
    x[last, :] = dot6(system[last, :], x[pl.ds(0, n), :])


def mixing_kernel(products, sums, high, low, x, system, r, parts, both):
    n = products.shape[0]
    square = jnp.sum(sums[1:2, 0:1] / sums[1:2, 1:2])
    inflation = jnp.sqrt(jnp.full((1, n), square, jnp.float32))

    def traced(rows, trace):
        eye = unit(rows, TILE, rows.start)
        return trace + jnp.sum(eye * products[rows, rows], axis=0, keepdims=True)

    trace = jnp.sum(by_rows(n, traced, jnp.zeros((1, TILE), jnp.float32))) * square
    shift = trace / ((n - 1.0) * n)

    def scaled(rows, most):
        s = unit(rows, n) + (products[rows, :] * square + shift)
        system[rows, :] = s
        return most + jnp.sum(jnp.abs(s), axis=0, keepdims=True)

    most = jnp.max(by_rows(n, scaled, jnp.zeros((1, n), jnp.float32)))
    first = lax.broadcasted_iota(jnp.int32, (EXTRA, n), 0) == 0
    system[pl.ds(n, EXTRA), :] = jnp.where(first, sums[0:1, :], 0.0)
    left = lax.cond(
        most < WELL_CONDITIONED,
        lambda: quick_inverse(x, system, r, parts, both),
        lambda: jnp.float32(1.0),
    )

    @pl.when(jnp.logical_not(left <= ROUNDING))
    def _():
        pl.run_scoped(
            lambda tmp: careful_inverse(x, system, r, tmp), pltpu.VMEM((n, n), jnp.float32)
        )

    q = x[pl.ds(n, 1), :] * square

    def mix(rows, _):
        eye = unit(rows, n)
        mixing = (0.5 * inflation) * (eye + x[rows, :]) + q
        mean = jnp.sum(mixing, axis=1, keepdims=True) * (1.0 / n)
        high[rows, :], low[rows, :] = split_bf16(mixing - mean + 1.0 / n)
        return 0

    by_rows(n, mix, 0)


def mixed(products, sums):
    n = products.shape[0]
    return pl.pallas_call(
        mixing_kernel,
        name="mixing",
        out_shape=[jax.ShapeDtypeStruct((n, n), jnp.bfloat16)] * 2,
        in_specs=[VMEM, VMEM],
        out_specs=[VMEM, VMEM],
        scratch_shapes=[
            pltpu.VMEM((n + EXTRA, n), jnp.float32),
            pltpu.VMEM((n + EXTRA, n), jnp.float32),
            pltpu.VMEM((n, n), jnp.float32),
            pltpu.VMEM((2 * (n + EXTRA), n), jnp.bfloat16),
            pltpu.VMEM((2 * n, n), jnp.bfloat16),
        ],
    )(products, sums)


def put_out_kernel(own, out, done):
    copy = pltpu.make_async_copy(own, out, done)
    copy.start()
    copy.wait()


def put_out(own):
    return pl.pallas_call(
        put_out_kernel,
        name="put_out",
        out_shape=jax.ShapeDtypeStruct(own.shape, own.dtype),
        in_specs=[VMEM],
        out_specs=pl.BlockSpec(memory_space=pl.ANY),
        scratch_shapes=[pltpu.SemaphoreType.DMA],
    )(own)


def local(ensemble, obs_offset, observed, obs_var):
    state, products, sums = gathered(ensemble, obs_offset, observed, obs_var)
    high, low = mixed(products, sums)
    return put_out(scattered(high, low, state.reshape(len(products), -1), len(ensemble)))


def solution(mesh):
    finer = Mesh(
        mesh.devices.reshape(4, 8, 2, mesh.shape["region"]),
        ("member_0", "member_1", "member_2", "region"),
    )
    in_specs = (
        P(MEMBER_REGION, None),
        P("region", MEMBER, None),
        P("region", MEMBER, None),
        P("region", MEMBER, None),
    )
    out_specs = P(MEMBER_REGION, None)
    return jax.shard_map(local, mesh=finer, in_specs=in_specs, out_specs=out_specs, check_vma=False)
```

```python
import jax
import jax.numpy as jnp
from jax import lax
from jax.experimental import pallas as pl
from jax.experimental.pallas import tpu as pltpu
from jax.sharding import Mesh
from jax.sharding import PartitionSpec as P

MEMBER = ("member_0", "member_1", "member_2")
MEMBER_REGION = ("member_0", "member_1", "member_2", "region")


MESH_ID = pl.DeviceIdType.MESH
SIDE_Y, SIDE_Z, CORES, SIDE_X = 4, 8, 2, 4
TILE = 128


def here():
    return (
        lax.axis_index("region"),
        lax.axis_index("member_0"),
        lax.axis_index("member_1"),
        lax.axis_index("member_2"),
    )


def device(x, y, z, c):
    return (y, z, c, x)


def chip_peer(i):
    x, y, z, c = here()
    return lax.rem(x + i, SIDE_X), lax.rem(y + i // SIDE_X, SIDE_Y), z, c


def in_plane(i):
    return lax.rem(i // 4, 4), lax.rem(i // 16, 2), lax.rem(i, 4)


PLANE = SIDE_X * SIDE_Y * CORES


def plane_peer(i):
    x, y, z, c = here()
    dy, dc, dx = in_plane(i)
    return lax.rem(x + dx, SIDE_X), lax.rem(y + dy, SIDE_Y), z, lax.rem(c + dc, CORES)


def line_peer(i):
    x, y, z, c = here()
    return x, y, lax.rem(z + i, SIDE_Z), c


def greet(barrier):
    @pl.loop(1, PLANE)
    def _(i):
        pl.semaphore_signal(barrier, 1, device_id=device(*plane_peer(i)), device_id_type=MESH_ID)

    @pl.loop(1, SIDE_Z)
    def _(i):
        pl.semaphore_signal(barrier, 1, device_id=device(*line_peer(i)), device_id_type=MESH_ID)


def met(barrier):
    pl.semaphore_wait(barrier, PLANE - 1 + SIDE_Z - 1)


def remote(src, dst, send, recv, place):
    return pltpu.make_async_remote_copy(
        src, dst, send, recv, device_id=device(*place), device_id_type=MESH_ID
    )


def block_of(x, y, z, c):
    return ((x * SIDE_Y + y) * SIDE_Z + z) * CORES + c


def links_of(block, size):
    return pl.ds(pl.multiple_of(block * size, size), size)


def no_matter(ref, send, recv):
    return remote(ref, ref, send, recv, here())


def dot6_t(a, b):
    return lax.dot_general(
        a,
        b,
        (((1,), (1,)), ((), ())),
        precision=lax.Precision.HIGHEST,
        preferred_element_type=jnp.float32,
    )


def along(k):
    d = k // 2 + 1
    return lax.rem(jnp.where(lax.rem(k, 2) == 0, d, SIDE_Z - d), SIDE_Z) * jnp.where(k == 7, 0, 1)


EARLY = 2


def gather_kernel(
    ensemble, offsets, observed, variances, whole, total, sums,
    own, notes, numbers, pieces, stage, all_notes, seen, picked, product, half, chunks, extras,
    other, copied, send, recv, arrived,
):
    x, y, z, c = here()
    size = own.shape[1] // (PLANE * SIDE_Z)
    members = sums.shape[1]
    seat = c * SIDE_X + x
    loads = [
        pltpu.make_async_copy(ensemble, own, copied.at[0]),
        pltpu.make_async_copy(offsets.at[0], numbers, copied.at[1]),
        pltpu.make_async_copy(observed.at[0], notes.at[pl.ds(1, 1), :], copied.at[2]),
        pltpu.make_async_copy(variances.at[0], notes.at[pl.ds(2, 1), :], copied.at[3]),
    ]
    for load in loads:
        load.start()
    barrier = pltpu.get_barrier_semaphore()
    greet(barrier)
    for load in loads:
        load.wait()
    notes[0:1, :] = numbers[...].astype(jnp.float32)
    count, watches = notes.shape[1], all_notes.shape[2]
    to = lax.broadcasted_iota(jnp.int32, (count, watches), 1)
    at = lax.broadcasted_iota(jnp.int32, (count, watches), 0) + z * count
    row = lax.broadcasted_iota(jnp.int32, (8, count), 0)
    placed = dot6(
        jnp.where(row < 3, notes[...], 0.0), jnp.where(to == at, 1.0, 0.0).astype(jnp.float32)
    )
    mine = all_notes.at[SIDE_Z]
    mine[...] = placed

    @pl.loop(0, SIDE_Z)
    def _(t):
        pieces[t, y, seat] = own[:, links_of(block_of(x, y, t, c), size)]

    met(barrier)

    @pl.loop(1, SIDE_Z)
    def _(i):
        remote(mine, all_notes.at[z], send.at[0], recv.at[0], line_peer(i)).start()

    @pl.loop(0, SIDE_Z)
    def _(k):
        t = lax.rem(z + along(k), SIDE_Z)

        @pl.loop(1, PLANE)
        def _(i):
            px, py, _, pc = plane_peer(i)
            remote(
                own.at[:, links_of(block_of(px, py, t, pc), size)],
                pieces.at[t, y, seat],
                send.at[1],
                arrived.at[t],
                (px, py, z, pc),
            ).start()

    all_notes[z] = placed
    no_matter(all_notes.at[pl.ds(0, SIDE_Z - 1)], send.at[0], recv.at[0]).wait()
    table = jnp.sum(all_notes[pl.ds(0, SIDE_Z)], axis=0)
    offset = table[0:1, :].astype(jnp.int32)
    measured = table[1:2, :]
    variance = table[2:3, :]
    link = lax.broadcasted_iota(jnp.int32, (size, watches), 0)
    seen[...] = jnp.where(link == offset, 1.0, 0.0).astype(jnp.bfloat16)
    line = lax.broadcasted_iota(jnp.int32, (members // SIDE_Z, watches), 1) // count

    def pass_on(k):
        t = lax.rem(z + along(k), SIDE_Z)
        remote(stage.at[t], whole.at[:, z], send.at[3], recv.at[3], (x, y, t, c)).start()

    def pick(k, found):
        t = lax.rem(z + along(k), SIDE_Z)
        no_matter(
            own.at[:, pl.ds(0, (PLANE - 1) * size)], send.at[1], arrived.at[t]
        ).wait_recv()

        def lay(j, _):
            stage[t, j] = pieces[t, j].reshape(stage.shape[2:])
            return 0

        lax.fori_loop(0, SIDE_Y, lay, 0)
        rows = stage[t].reshape(members // SIDE_Z, size)
        values = jnp.dot(rows, seen[...], preferred_element_type=jnp.float32)

        @pl.when(jnp.logical_and(k >= 1, k <= EARLY))
        def _():
            pass_on(k - 1)

        return jnp.where(line == t, values, found)

    found = lax.fori_loop(0, SIDE_Z, pick, jnp.zeros(line.shape, jnp.float32))
    mine = picked.at[SIDE_Z]
    mine[...] = found.astype(jnp.bfloat16).reshape(mine.shape)

    @pl.loop(1, SIDE_Z)
    def _(i):
        remote(mine, picked.at[z], send.at[2], recv.at[2], line_peer(i)).start()

    @pl.loop(EARLY, SIDE_Z - 1)
    def _(k):
        pass_on(k)

    picked[z] = mine[...]
    whole[:, z] = stage[z]
    no_matter(
        own.at[:, pl.ds(0, (PLANE - 1) * SIDE_Z * size)], send.at[1], recv.at[1]
    ).wait_send()
    no_matter(picked.at[pl.ds(0, SIDE_Z - 1)], send.at[2], recv.at[2]).wait()

    values = jnp.swapaxes(picked[pl.ds(0, SIDE_Z)], 0, 1).reshape(members, watches)
    values = values.astype(jnp.float32)
    center = jnp.sum(values, axis=0, keepdims=True) * (1.0 / members)
    anomaly = values - center
    innovation = measured - center
    weight = 1.0 / ((members - 1.0) * variance)
    spread = jnp.sum(anomaly * anomaly, axis=0, keepdims=True) * (1.0 / (members - 1.0)) + variance
    column = dot6_t(weight * innovation, anomaly)
    numer = jnp.sum(innovation * innovation, axis=1, keepdims=True)
    denom = jnp.sum(spread, axis=1, keepdims=True)
    lane = lax.broadcasted_iota(jnp.int32, column.shape, 1)
    extra = extras.at[PLANE]
    extra[0:1, :] = column
    extra[1:2, :] = jnp.where(lane == 0, numer, jnp.where(lane == 1, denom, 0.0))
    weighted = anomaly * weight
    block = 0
    for i in range(members // TILE):
        row = dot6_t(weighted[i * TILE : (i + 1) * TILE], anomaly[: (i + 1) * TILE])
        for j in range(i + 1):
            core, at = divmod(block, product.shape[1] // TILE)
            product[core, at * TILE : (at + 1) * TILE, :] = row[:, j * TILE : (j + 1) * TILE]
            block += 1

    rows = product.shape[1]
    partner = (x, y, z, 1 - c)
    remote(product.at[1 - c], other, send.at[4], recv.at[4], partner).start()

    @pl.loop(1, PLANE)
    def _(i):
        remote(
            extra, extras.at[y * (CORES * SIDE_X) + seat], send.at[5], recv.at[5], plane_peer(i)
        ).start()

    extras[y * (CORES * SIDE_X) + seat] = extra[...]
    no_matter(other, send.at[4], recv.at[4]).wait()
    half[...] = product[c] + other[...]
    chips = SIDE_X * SIDE_Y
    part = rows // chips

    def part_of(px, py):
        return pl.ds(pl.multiple_of((py * SIDE_X + px) * part, part), part)

    @pl.loop(1, chips)
    def _(i):
        place = chip_peer(i)
        remote(
            half.at[part_of(place[0], place[1])],
            chunks.at[y * SIDE_X + x],
            send.at[6],
            recv.at[6],
            place,
        ).start()

    chunks[y * SIDE_X + x] = half[part_of(x, y), :]
    no_matter(chunks.at[pl.ds(0, chips - 1)], send.at[6], recv.at[6]).wait()
    done = total.at[c, part_of(x, y)]
    done[...] = jnp.sum(chunks[...], axis=0)

    @pl.loop(1, chips)
    def _(i):
        remote(done, done, send.at[7], recv.at[7], chip_peer(i)).start()

    no_matter(half.at[pl.ds(0, rows - part)], send.at[7], recv.at[7]).wait()
    remote(total.at[c], total.at[c], send.at[8], recv.at[8], partner).start()
    no_matter(extras.at[pl.ds(0, PLANE - 1)], send.at[5], recv.at[5]).wait()
    sums[...] = jnp.sum(extras[pl.ds(0, PLANE)], axis=0)
    no_matter(other, send.at[8], recv.at[8]).wait()
    no_matter(stage.at[pl.ds(0, SIDE_Z - 1)], send.at[3], recv.at[3]).wait()


def scatter_kernel(high, low, state, own, whole, stage, send_z, recv_z, send_p, recv_p):
    x, y, z, c = here()
    rows, size = state.shape
    barrier = pltpu.get_barrier_semaphore()
    greet(barrier)
    wide = 256

    @pl.loop(0, size // wide)
    def _(k):
        at = links_of(k, wide)
        values = dot1(high[...], state[:, at]) + dot1(low[...], state[:, at])
        whole[:, :, :, :, at] = values.astype(jnp.bfloat16).reshape(*whole.shape[:-1], wide)

    met(barrier)

    @pl.loop(0, SIDE_Z - 1)
    def _(k):
        t = lax.rem(z + along(k), SIDE_Z)

        @pl.loop(0, SIDE_Y)
        def _(dy):
            py = lax.rem(y + dy, SIDE_Y)
            remote(
                whole.at[py, t], stage.at[z, py], send_z, recv_z.at[z, py], (x, y, t, c)
            ).start()

    def hand_on(source, py, dy, block):
        @pl.loop(jnp.where(dy == 0, 1, 0), CORES * SIDE_X)
        def _(j):
            px = lax.rem(x + lax.rem(j, SIDE_X), SIDE_X)
            pc = lax.rem(c + j // SIDE_X, CORES)
            remote(
                source.at[pc * SIDE_X + px],
                own.at[:, links_of(block, size)],
                send_p,
                recv_p,
                (px, py, z, pc),
            ).start()

        @pl.when(dy == 0)
        def _():
            own[:, links_of(block, size)] = source[c * SIDE_X + x]

    @pl.loop(0, SIDE_Y)
    def _(dy):
        py = lax.rem(y + dy, SIDE_Y)
        hand_on(whole.at[py, z], py, dy, block_of(x, y, z, c))

    @pl.loop(0, SIDE_Z - 1)
    def _(k):
        t = lax.rem(z + SIDE_Z - along(k), SIDE_Z)

        @pl.loop(0, SIDE_Y)
        def _(dy):
            py = lax.rem(y + dy, SIDE_Y)
            no_matter(stage.at[t, py], send_z, recv_z.at[t, py]).wait_recv()
            hand_on(stage.at[t, py], py, dy, block_of(x, y, t, c))

    no_matter(stage.at[pl.ds(0, SIDE_Z - 1)], send_z, recv_z.at[0, 0]).wait_send()
    no_matter(own.at[:, pl.ds(0, (PLANE - 1) * SIDE_Z * size)], send_p, recv_p).wait()


VMEM = pl.BlockSpec(memory_space=pltpu.VMEM)
ROOM = 24 << 20


def gathered(own, offsets, observed, variances):
    rows = own.shape[0]
    size = own.shape[1] // (PLANE * SIDE_Z)
    members = rows * PLANE * SIDE_Z
    seats = CORES * SIDE_X
    count = offsets.shape[-1]
    watches = SIDE_Z * count
    tiles = members // TILE
    packed = tiles * (tiles + 1) // 2 * TILE // CORES
    part = packed // (SIDE_X * SIDE_Y)
    f32, bf16 = jnp.float32, jnp.bfloat16
    return pl.pallas_call(
        gather_kernel,
        name="gather",
        out_shape=(
            jax.ShapeDtypeStruct((SIDE_Y, SIDE_Z, seats * rows, size), bf16),
            jax.ShapeDtypeStruct((CORES, packed, TILE), f32),
            jax.ShapeDtypeStruct((2, members), f32),
        ),
        in_specs=[pl.BlockSpec(memory_space=pltpu.HBM)] * 4,
        out_specs=(VMEM, VMEM, VMEM),
        scratch_shapes=[
            pltpu.VMEM(own.shape, bf16),
            pltpu.VMEM((8, count), f32),
            pltpu.VMEM((1, count), jnp.int32),
            pltpu.VMEM((SIDE_Z, SIDE_Y, seats, rows, size), bf16),
            pltpu.VMEM((SIDE_Z, SIDE_Y, seats * rows, size), bf16),
            pltpu.VMEM((SIDE_Z + 1, 8, watches), f32),
            pltpu.VMEM((size, watches), bf16),
            pltpu.VMEM((SIDE_Z + 1, SIDE_Y, seats * rows, watches), bf16),
            pltpu.VMEM((CORES, packed, TILE), f32),
            pltpu.VMEM((packed, TILE), f32),
            pltpu.VMEM((SIDE_X * SIDE_Y, part, TILE), f32),
            pltpu.VMEM((PLANE + 1, 2, members), f32),
            pltpu.VMEM((packed, TILE), f32),
            pltpu.SemaphoreType.DMA((4,)),
            pltpu.SemaphoreType.DMA((9,)),
            pltpu.SemaphoreType.DMA((9,)),
            pltpu.SemaphoreType.DMA((SIDE_Z,)),
        ],
        compiler_params=pltpu.CompilerParams(
            collective_id=0, has_side_effects=True, vmem_limit_bytes=ROOM
        ),
    )(*(pltpu.with_memory_space_constraint(a, pltpu.HBM) for a in (own, offsets, observed, variances)))


def scattered(high, low, state, own_rows):
    rows, size = state.shape
    shape = (SIDE_Y, SIDE_Z, CORES * SIDE_X, own_rows, size)
    return pl.pallas_call(
        scatter_kernel,
        name="scatter",
        out_shape=jax.ShapeDtypeStruct((own_rows, size * PLANE * SIDE_Z), state.dtype),
        in_specs=[VMEM, VMEM, VMEM],
        out_specs=VMEM,
        scratch_shapes=[
            pltpu.VMEM(shape, state.dtype),
            pltpu.VMEM((SIDE_Z, SIDE_Y, *shape[2:]), state.dtype),
            pltpu.SemaphoreType.DMA,
            pltpu.SemaphoreType.DMA((SIDE_Z, SIDE_Y)),
            pltpu.SemaphoreType.DMA,
            pltpu.SemaphoreType.DMA,
        ],
        compiler_params=pltpu.CompilerParams(
            collective_id=1, has_side_effects=True, vmem_limit_bytes=ROOM
        ),
    )(high, low, state)


def split_bf16(a):
    high = a.astype(jnp.bfloat16)
    return high, (a - high.astype(jnp.float32)).astype(jnp.bfloat16)


def dot1(a, b):
    return jnp.dot(
        a.astype(jnp.bfloat16), b.astype(jnp.bfloat16), preferred_element_type=jnp.float32
    )


def dot6(a, b):
    return jnp.dot(a, b, precision=lax.Precision.HIGHEST, preferred_element_type=jnp.float32)


WELL_CONDITIONED = 2000.0
ROUNDING = 1e-6


def by_rows(rows, body, init=None):
    def step(i, carry):
        return body(pl.ds(pl.multiple_of(i * TILE, TILE), TILE), carry)

    return lax.fori_loop(0, rows // TILE, step, init)


def largest_row(m):
    return jnp.max(jnp.sum(jnp.abs(m), axis=1))


def sum_of_squares(m):
    return jnp.sum(m * m)


def unit(rows, n):
    row = lax.broadcasted_iota(jnp.int32, (TILE, n), 0) + rows.start
    col = lax.broadcasted_iota(jnp.int32, (TILE, n), 1)
    return jnp.where(row == col, 1.0, 0.0).astype(jnp.float32)


EXTRA = 16


def residual_squares(left):
    return jnp.sum(jnp.sum(left * left, axis=0, keepdims=True))


def quick_inverse(x, system, r, parts, both):
    n = system.shape[1]
    rows = system.shape[0]

    def passes(lhs, rhs):
        return jnp.dot(lhs, rhs, preferred_element_type=jnp.float32)

    values = system[...]
    high = values.astype(jnp.bfloat16)
    parts[pl.ds(0, rows), :] = high
    parts[pl.ds(rows, rows), :] = (values - high.astype(jnp.float32)).astype(jnp.bfloat16)
    top = pl.ds(0, n)
    r[...] = passes(parts[top, :], parts[top, :])
    bound = jnp.sqrt(jnp.max(jnp.sum(jnp.abs(r[...]), axis=0, keepdims=True)) * 1.02)
    a = 2.0 / (1.0 + bound)

    def first(rows, total):
        eye = unit(rows, n)
        s = system[rows, :] * a
        left = eye - 2.0 * s + (a * a) * r[rows, :]
        grown = a * (2.0 * eye - s)
        x[rows, :] = grown
        both[rows, :] = grown.astype(jnp.bfloat16)
        both[pl.ds(n + rows.start, TILE), :] = left.astype(jnp.bfloat16)
        return total + jnp.sum(left * left, axis=0, keepdims=True)

    total = by_rows(n, first, jnp.zeros((1, n), jnp.float32))

    def more(state):
        count, size = state
        return jnp.logical_and(count < 16, size > 0.01)

    def double(state):
        count, _ = state
        out = passes(both[...], both[pl.ds(n, n), :])
        grown = x[top, :] + out[:n]
        left = out[n:]
        x[top, :] = grown
        both[...] = jnp.concatenate([grown, left]).astype(jnp.bfloat16)
        return count + 1, residual_squares(left)

    lax.while_loop(more, double, (jnp.int32(0), jnp.sum(total)))

    def more_newton(state):
        count, size = state
        return jnp.logical_and(count < 8, size > ROUNDING)

    def newton(state):
        count, _ = state
        now = x[top, :]
        xh = now.astype(jnp.bfloat16)
        xl = (now - xh.astype(jnp.float32)).astype(jnp.bfloat16)
        here_high = parts[pl.ds(0, rows), :]
        out = passes(here_high, xh) + (
            passes(here_high, xl) + passes(parts[pl.ds(rows, rows), :], xh)
        )
        r[...] = out[:n]

        def left_of(at, total):
            left = unit(at, n) - r[at, :]
            both[at, :] = left.astype(jnp.bfloat16)
            return total + jnp.sum(left * left, axis=0, keepdims=True)

        total = by_rows(n, left_of, jnp.zeros((1, n), jnp.float32))
        tail = out[n:]
        grown = jnp.concatenate([now, tail])
        x[...] = grown + passes(jnp.concatenate([xh, tail.astype(jnp.bfloat16)]), both[top, :])
        return count + 1, jnp.sum(total)

    return lax.while_loop(more_newton, newton, (jnp.int32(0), jnp.float32(1.0)))[1]


def careful_inverse(x, system, r, tmp):
    n = system.shape[1]

    def square(rows, bound):
        tmp[rows, :] = dot6(system[rows, :], system[pl.ds(0, n), :])
        return jnp.maximum(bound, largest_row(tmp[rows, :]))

    bound = jnp.sqrt(by_rows(n, square, jnp.float32(0.0)) * 1.02)
    a = 2.0 / (1.0 + bound)

    def first(rows, total):
        eye = unit(rows, n)
        s = system[rows, :] * a
        x[rows, :] = a * (2.0 * eye - s)
        left = eye - 2.0 * s + (a * a) * tmp[rows, :]
        r[rows, :] = left
        return total + sum_of_squares(left)

    def more(state):
        count, size = state
        return jnp.logical_and(count < 40, size > 4e-4)

    def double(state):
        def grow(rows, _):
            x[rows, :] += dot6(x[rows, :], r[...])
            tmp[rows, :] = dot6(r[rows, :], r[...])
            return 0

        by_rows(n, grow, 0)

        def take(rows, total):
            left = tmp[rows, :]
            r[rows, :] = left
            return total + sum_of_squares(left)

        return state[0] + 1, by_rows(n, take, jnp.float32(0.0))

    lax.while_loop(more, double, (jnp.int32(0), by_rows(n, first, jnp.float32(0.0))))

    def more_newton(state):
        count, size = state
        return jnp.logical_and(count < 12, size > ROUNDING)

    def newton(state):
        def residual(rows, total):
            left = unit(rows, n) - dot6(system[rows, :], x[pl.ds(0, n), :])
            r[rows, :] = left
            return total + sum_of_squares(left)

        size = by_rows(n, residual, jnp.float32(0.0))

        def correct(rows, _):
            x[rows, :] += dot6(x[rows, :], r[...])
            return 0

        by_rows(n, correct, 0)
        return state[0] + 1, size

    lax.while_loop(more_newton, newton, (jnp.int32(0), jnp.float32(1.0)))
    last = pl.ds(n, system.shape[0] - n)
    x[last, :] = dot6(system[last, :], x[pl.ds(0, n), :])


def mixing_kernel(products, sums, high, low, x, system, r, parts, both):
    n = sums.shape[1]
    tiles = n // TILE
    square = jnp.sum(sums[1:2, 0:1] / sums[1:2, 1:2])
    inflation = jnp.sqrt(jnp.full((1, n), square, jnp.float32))
    row = lax.broadcasted_iota(jnp.int32, (TILE, TILE), 0)
    col = lax.broadcasted_iota(jnp.int32, (TILE, TILE), 1)
    eye = jnp.where(row == col, 1.0, 0.0).astype(jnp.float32)
    corners = [i * (i + 3) // 2 for i in range(tiles)]
    diagonal = sum(products[block] for block in corners)
    trace = jnp.sum(jnp.sum(eye * diagonal, axis=0, keepdims=True)) * square
    shift = trace / ((n - 1.0) * n)
    block = 0
    for i in range(tiles):
        down = pl.ds(i * TILE, TILE)
        for j in range(i + 1):
            across = pl.ds(j * TILE, TILE)
            values = products[block] * square + shift
            if i == j:
                system[down, down] = values + eye
            else:
                system[down, across] = values
                system[across, down] = values.T
            block += 1

    def longest(rows, most):
        return most + jnp.sum(jnp.abs(system[rows, :]), axis=0, keepdims=True)

    most = jnp.max(by_rows(n, longest, jnp.zeros((1, n), jnp.float32)))
    first = lax.broadcasted_iota(jnp.int32, (EXTRA, n), 0) == 0
    system[pl.ds(n, EXTRA), :] = jnp.where(first, sums[0:1, :], 0.0)
    left = lax.cond(
        most < WELL_CONDITIONED,
        lambda: quick_inverse(x, system, r, parts, both),
        lambda: jnp.float32(1.0),
    )

    @pl.when(jnp.logical_not(left <= ROUNDING))
    def _():
        pl.run_scoped(
            lambda tmp: careful_inverse(x, system, r, tmp), pltpu.VMEM((n, n), jnp.float32)
        )

    q = x[pl.ds(n, 1), :] * square

    def mix(rows, _):
        eye = unit(rows, n)
        mixing = (0.5 * inflation) * (eye + x[rows, :]) + q
        mean = jnp.sum(mixing, axis=1, keepdims=True) * (1.0 / n)
        high[rows, :], low[rows, :] = split_bf16(mixing - mean + 1.0 / n)
        return 0

    by_rows(n, mix, 0)


def mixed(products, sums):
    n = sums.shape[1]
    return pl.pallas_call(
        mixing_kernel,
        name="mixing",
        out_shape=[jax.ShapeDtypeStruct((n, n), jnp.bfloat16)] * 2,
        in_specs=[VMEM, VMEM],
        out_specs=[VMEM, VMEM],
        scratch_shapes=[
            pltpu.VMEM((n + EXTRA, n), jnp.float32),
            pltpu.VMEM((n + EXTRA, n), jnp.float32),
            pltpu.VMEM((n, n), jnp.float32),
            pltpu.VMEM((2 * (n + EXTRA), n), jnp.bfloat16),
            pltpu.VMEM((2 * n, n), jnp.bfloat16),
        ],
        compiler_params=pltpu.CompilerParams(vmem_limit_bytes=ROOM),
    )(products.reshape(-1, TILE, TILE), sums)


def put_out_kernel(own, out, done):
    copy = pltpu.make_async_copy(own, out, done)
    copy.start()
    copy.wait()


def put_out(own):
    return pl.pallas_call(
        put_out_kernel,
        name="put_out",
        out_shape=jax.ShapeDtypeStruct(own.shape, own.dtype),
        in_specs=[VMEM],
        out_specs=pl.BlockSpec(memory_space=pltpu.HBM),
        scratch_shapes=[pltpu.SemaphoreType.DMA],
        compiler_params=pltpu.CompilerParams(vmem_limit_bytes=ROOM),
    )(own)


def local(ensemble, obs_offset, observed, obs_var):
    state, products, sums = gathered(ensemble, obs_offset, observed, obs_var)
    high, low = mixed(products, sums)
    return put_out(scattered(high, low, state.reshape(sums.shape[1], -1), len(ensemble)))


def solution(mesh):
    finer = Mesh(
        mesh.devices.reshape(4, 8, 2, mesh.shape["region"]),
        ("member_0", "member_1", "member_2", "region"),
    )
    in_specs = (
        P(MEMBER_REGION, None),
        P("region", MEMBER, None),
        P("region", MEMBER, None),
        P("region", MEMBER, None),
    )
    out_specs = P(MEMBER_REGION, None)
    return jax.shard_map(local, mesh=finer, in_specs=in_specs, out_specs=out_specs, check_vma=False)
```

```python
import jax
import jax.numpy as jnp
from jax import lax
from jax.experimental import pallas as pl
from jax.experimental.pallas import tpu as pltpu
from jax.sharding import Mesh
from jax.sharding import PartitionSpec as P

MEMBER = ("member_0", "member_1", "member_2")
MEMBER_REGION = ("member_0", "member_1", "member_2", "region")


MESH_ID = pl.DeviceIdType.MESH
SIDE_Y, SIDE_Z, CORES, SIDE_X = 4, 8, 2, 4
TILE = 128


def here():
    return (
        lax.axis_index("region"),
        lax.axis_index("member_0"),
        lax.axis_index("member_1"),
        lax.axis_index("member_2"),
    )


def device(x, y, z, c):
    return (y, z, c, x)


def chip_peer(i):
    x, y, z, c = here()
    i = lax.rem(i * 7, SIDE_X * SIDE_Y)
    return lax.rem(x + i, SIDE_X), lax.rem(y + i // SIDE_X, SIDE_Y), z, c


def in_plane(i):
    return lax.rem(i // 4, 4), lax.rem(i // 16, 2), lax.rem(i, 4)


PLANE = SIDE_X * SIDE_Y * CORES


def plane_peer(i):
    x, y, z, c = here()
    dy, dc, dx = in_plane(lax.rem(i * 13, PLANE))
    return lax.rem(x + dx, SIDE_X), lax.rem(y + dy, SIDE_Y), z, lax.rem(c + dc, CORES)


def line_peer(i):
    x, y, z, c = here()
    return x, y, lax.rem(z + i, SIDE_Z), c


def greet(barrier):
    @pl.loop(1, PLANE)
    def _(i):
        pl.semaphore_signal(barrier, 1, device_id=device(*plane_peer(i)), device_id_type=MESH_ID)

    @pl.loop(1, SIDE_Z)
    def _(i):
        pl.semaphore_signal(barrier, 1, device_id=device(*line_peer(i)), device_id_type=MESH_ID)


def met(barrier):
    pl.semaphore_wait(barrier, PLANE - 1 + SIDE_Z - 1)


def remote(src, dst, send, recv, place):
    return pltpu.make_async_remote_copy(
        src, dst, send, recv, device_id=device(*place), device_id_type=MESH_ID
    )


def block_of(x, y, z, c):
    return ((x * SIDE_Y + y) * SIDE_Z + z) * CORES + c


def links_of(block, size):
    return pl.ds(pl.multiple_of(block * size, size), size)


def no_matter(ref, send, recv):
    return remote(ref, ref, send, recv, here())


def dot6_t(a, b):
    return lax.dot_general(
        a,
        b,
        (((1,), (1,)), ((), ())),
        precision=lax.Precision.HIGHEST,
        preferred_element_type=jnp.float32,
    )


def along(k):
    d = k // 2 + 1
    return lax.rem(jnp.where(lax.rem(k, 2) == 0, d, SIDE_Z - d), SIDE_Z) * jnp.where(k == 7, 0, 1)


EARLY = 2
HALFWAY = 4


def gather_kernel(
    ensemble, offsets, observed, variances, whole, total, sums,
    own, notes, numbers, pieces, stage, all_notes, seen, picked, product, half, chunks, extras,
    other, copied, send, recv, arrived, parted,
):
    x, y, z, c = here()
    size = own.shape[1] // (PLANE * SIDE_Z)
    members = sums.shape[1]
    seat = c * SIDE_X + x
    loads = [
        pltpu.make_async_copy(ensemble, own, copied.at[0]),
        pltpu.make_async_copy(offsets.at[0], numbers, copied.at[1]),
        pltpu.make_async_copy(observed.at[0], notes.at[pl.ds(1, 1), :], copied.at[2]),
        pltpu.make_async_copy(variances.at[0], notes.at[pl.ds(2, 1), :], copied.at[3]),
    ]
    for load in loads:
        load.start()
    barrier = pltpu.get_barrier_semaphore()
    greet(barrier)
    for load in loads:
        load.wait()
    notes[0:1, :] = numbers[...].astype(jnp.float32)
    count, watches = notes.shape[1], all_notes.shape[2]
    to = lax.broadcasted_iota(jnp.int32, (count, watches), 1)
    at = lax.broadcasted_iota(jnp.int32, (count, watches), 0) + z * count
    row = lax.broadcasted_iota(jnp.int32, (8, count), 0)
    placed = dot6(
        jnp.where(row < 3, notes[...], 0.0), jnp.where(to == at, 1.0, 0.0).astype(jnp.float32)
    )
    mine = all_notes.at[SIDE_Z]
    mine[...] = placed

    @pl.loop(0, SIDE_Z)
    def _(t):
        pieces[t, y, seat] = own[:, links_of(block_of(x, y, t, c), size)]

    met(barrier)

    @pl.loop(1, SIDE_Z)
    def _(i):
        remote(mine, all_notes.at[z], send.at[0], recv.at[0], line_peer(i)).start()

    @pl.loop(0, SIDE_Z)
    def _(k):
        t = lax.rem(z + along(k), SIDE_Z)

        @pl.loop(1, PLANE)
        def _(i):
            px, py, _, pc = plane_peer(i)
            remote(
                own.at[:, links_of(block_of(px, py, t, pc), size)],
                pieces.at[t, y, seat],
                send.at[1],
                arrived.at[t],
                (px, py, z, pc),
            ).start()

    all_notes[z] = placed
    no_matter(all_notes.at[pl.ds(0, SIDE_Z - 1)], send.at[0], recv.at[0]).wait()
    table = jnp.sum(all_notes[pl.ds(0, SIDE_Z)], axis=0)
    offset = table[0:1, :].astype(jnp.int32)
    measured = table[1:2, :]
    variance = table[2:3, :]
    link = lax.broadcasted_iota(jnp.int32, (size, watches), 0)
    seen[...] = jnp.where(link == offset, 1.0, 0.0).astype(jnp.bfloat16)
    line = lax.broadcasted_iota(jnp.int32, (members // SIDE_Z, watches), 1) // count

    def pass_on(k):
        t = lax.rem(z + along(k), SIDE_Z)
        remote(stage.at[t], whole.at[:, z], send.at[3], recv.at[3], (x, y, t, c)).start()

    def pick(k, found):
        t = lax.rem(z + along(k), SIDE_Z)
        no_matter(
            own.at[:, pl.ds(0, (PLANE - 1) * size)], send.at[1], arrived.at[t]
        ).wait_recv()

        def lay(j, _):
            stage[t, j] = pieces[t, j].reshape(stage.shape[2:])
            return 0

        lax.fori_loop(0, SIDE_Y, lay, 0)
        rows = stage[t].reshape(members // SIDE_Z, size)
        values = jnp.dot(rows, seen[...], preferred_element_type=jnp.float32)

        @pl.when(jnp.logical_and(k >= 1, k <= EARLY))
        def _():
            pass_on(k - 1)

        return jnp.where(line == t, values, found)

    found = lax.fori_loop(0, SIDE_Z, pick, jnp.zeros(line.shape, jnp.float32))
    mine = picked.at[SIDE_Z]
    mine[...] = found.astype(jnp.bfloat16).reshape(mine.shape)

    @pl.loop(1, SIDE_Z)
    def _(i):
        remote(mine, picked.at[z], send.at[2], recv.at[2], line_peer(i)).start()

    @pl.loop(EARLY, SIDE_Z - 1)
    def _(k):
        pass_on(k)

    picked[z] = mine[...]
    whole[:, z] = stage[z]
    no_matter(
        own.at[:, pl.ds(0, (PLANE - 1) * SIDE_Z * size)], send.at[1], recv.at[1]
    ).wait_send()
    no_matter(picked.at[pl.ds(0, SIDE_Z - 1)], send.at[2], recv.at[2]).wait()

    values = jnp.swapaxes(picked[pl.ds(0, SIDE_Z)], 0, 1).reshape(members, watches)
    values = values.astype(jnp.float32)
    center = jnp.sum(values, axis=0, keepdims=True) * (1.0 / members)
    anomaly = values - center
    innovation = measured - center
    weight = 1.0 / ((members - 1.0) * variance)
    spread = jnp.sum(anomaly * anomaly, axis=0, keepdims=True) * (1.0 / (members - 1.0)) + variance
    column = dot6_t(weight * innovation, anomaly)
    numer = jnp.sum(innovation * innovation, axis=1, keepdims=True)
    denom = jnp.sum(spread, axis=1, keepdims=True)
    lane = lax.broadcasted_iota(jnp.int32, column.shape, 1)
    extra = extras.at[PLANE]
    extra[0:1, :] = column
    extra[1:2, :] = jnp.where(lane == 0, numer, jnp.where(lane == 1, denom, 0.0))
    weighted = anomaly * weight
    block = 0
    for i in range(members // TILE):
        row = dot6_t(weighted[i * TILE : (i + 1) * TILE], anomaly[: (i + 1) * TILE])
        for j in range(i + 1):
            core, at = divmod(block, product.shape[1] // TILE)
            product[core, at * TILE : (at + 1) * TILE, :] = row[:, j * TILE : (j + 1) * TILE]
            block += 1

    rows = product.shape[1]
    partner = (x, y, z, 1 - c)
    remote(product.at[1 - c], other, send.at[4], recv.at[4], partner).start()

    @pl.loop(1, PLANE)
    def _(i):
        remote(
            extra, extras.at[y * (CORES * SIDE_X) + seat], send.at[5], recv.at[5], plane_peer(i)
        ).start()

    extras[y * (CORES * SIDE_X) + seat] = extra[...]
    no_matter(other, send.at[4], recv.at[4]).wait()
    half[...] = product[c] + other[...]
    chips = SIDE_X * SIDE_Y
    part = rows // chips

    def part_of(px, py):
        return pl.ds(pl.multiple_of((py * SIDE_X + px) * part, part), part)

    @pl.loop(1, chips)
    def _(i):
        place = chip_peer(i)
        remote(
            half.at[part_of(place[0], place[1])],
            chunks.at[y * SIDE_X + x],
            send.at[6],
            recv.at[6],
            place,
        ).start()

    chunks[y * SIDE_X + x] = half[part_of(x, y), :]
    no_matter(chunks.at[pl.ds(0, chips - 1)], send.at[6], recv.at[6]).wait()
    done = total.at[c, part_of(x, y)]
    done[...] = jnp.sum(chunks[...], axis=0)

    @pl.loop(1, chips)
    def _(i):
        place = chip_peer(i)
        remote(done, done, send.at[7], parted.at[y * SIDE_X + x], place).start()

    remote(done, done, send.at[8], recv.at[8], partner).start()

    @pl.loop(1, chips)
    def _(i):
        px, py, _, _ = chip_peer(chips - i)
        piece = total.at[c, part_of(px, py)]
        no_matter(piece, send.at[7], parted.at[py * SIDE_X + px]).wait_recv()
        remote(piece, piece, send.at[8], recv.at[8], partner).start()

    no_matter(half.at[pl.ds(0, rows - part)], send.at[7], recv.at[7]).wait_send()
    no_matter(extras.at[pl.ds(0, PLANE - 1)], send.at[5], recv.at[5]).wait()
    sums[...] = jnp.sum(extras[pl.ds(0, PLANE)], axis=0)
    no_matter(other, send.at[8], recv.at[8]).wait()
    no_matter(stage.at[pl.ds(0, SIDE_Z - 1)], send.at[3], recv.at[3]).wait()


def scatter_kernel(
    high, low, state, own, whole, far, near, send_far, arrived, send_near, recv_near,
    send_last, recv_last, send_own, recv_own,
):
    x, y, z, c = here()
    rows, size = state.shape
    chip, seat = x * SIDE_Y + y, c * SIDE_X + x
    cut = far.shape[-1]
    first, second = pl.ds(0, cut), pl.ds(cut, size - cut)
    barrier = pltpu.get_barrier_semaphore()
    greet(barrier)
    wide = 256

    @pl.loop(0, size // wide)
    def _(k):
        at = links_of(k, wide)
        values = dot1(high[...], state[:, at]) + dot1(low[...], state[:, at])
        whole[:, :, :, :, at] = values.astype(jnp.bfloat16).reshape(*whole.shape[:-1], wide)

    met(barrier)

    @pl.loop(0, SIDE_Z - 1)
    def _(k):
        t = lax.rem(z + along(k), SIDE_Z)

        @pl.loop(0, SIDE_Y)
        def _(dy):
            py = lax.rem(y + dy, SIDE_Y)
            remote(
                whole.at[py, t, :, :, first],
                far.at[z * SIDE_Y + py],
                send_far,
                arrived.at[z, py],
                (x, y, t, c),
            ).start()

    @pl.loop(1, PLANE)
    def _(i):
        px, py, _, pc = plane_peer(i)
        remote(
            whole.at[py, :, pc * SIDE_X + px, :, second],
            near.at[:, chip, c],
            send_near,
            recv_near,
            (px, py, z, pc),
        ).start()

    def hand_on(source, py, dy, t):
        @pl.loop(jnp.where(dy == 0, 1, 0), CORES * SIDE_X)
        def _(j):
            px = lax.rem(x + lax.rem(j, SIDE_X), SIDE_X)
            pc = lax.rem(c + j // SIDE_X, CORES)
            remote(
                source(pc * SIDE_X + px),
                own.at[chip, t, c, :, first],
                send_last,
                recv_last,
                (px, py, z, pc),
            ).start()

        @pl.when(dy == 0)
        def _():
            own[chip, t, c, :, first] = source(seat)[...]

    @pl.loop(0, SIDE_Y)
    def _(dy):
        py = lax.rem(y + dy, SIDE_Y)
        hand_on(lambda s: whole.at[py, z, s, :, first], py, dy, z)

    @pl.loop(0, SIDE_Z)
    def _(t):
        near[t, chip, c] = whole[y, t, seat, :, second]

    def take(k):
        t = lax.rem(z + SIDE_Z - along(k), SIDE_Z)

        @pl.loop(0, SIDE_Y)
        def _(dy):
            py = lax.rem(y + dy, SIDE_Y)
            no_matter(far.at[t * SIDE_Y + py], send_far, arrived.at[t, py]).wait_recv()
            hand_on(lambda s: far.at[t * SIDE_Y + py, s], py, dy, t)

    pl.loop(0, HALFWAY)(take)
    chips = SIDE_X * SIDE_Y
    others = far.at[pl.ds(0, PLANE - 1)]
    no_matter(others, send_near, recv_near).wait()

    @pl.loop(0, SIDE_Z - 1)
    def _(k):
        t = lax.rem(z + along(k), SIDE_Z)
        remote(
            near.at[t], own.at[:, z, :, :, second], send_own, recv_own, (x, y, t, c)
        ).start()

    @pl.loop(0, chips)
    def _(i):
        own[i, z, :, :, second] = near[z, i]

    pl.loop(HALFWAY, SIDE_Z - 1)(take)
    no_matter(far.at[pl.ds(0, (SIDE_Z - 1) * SIDE_Y)], send_far, recv_near).wait_send()
    no_matter(near.at[pl.ds(0, SIDE_Z - 1)], send_own, recv_own).wait()
    no_matter(others, send_last, recv_last).wait()


VMEM = pl.BlockSpec(memory_space=pltpu.VMEM)
ROOM = 24 << 20


def gathered(own, offsets, observed, variances):
    rows = own.shape[0]
    size = own.shape[1] // (PLANE * SIDE_Z)
    members = rows * PLANE * SIDE_Z
    seats = CORES * SIDE_X
    count = offsets.shape[-1]
    watches = SIDE_Z * count
    tiles = members // TILE
    packed = tiles * (tiles + 1) // 2 * TILE // CORES
    part = packed // (SIDE_X * SIDE_Y)
    f32, bf16 = jnp.float32, jnp.bfloat16
    return pl.pallas_call(
        gather_kernel,
        name="gather",
        out_shape=(
            jax.ShapeDtypeStruct((SIDE_Y, SIDE_Z, seats * rows, size), bf16),
            jax.ShapeDtypeStruct((CORES, packed, TILE), f32),
            jax.ShapeDtypeStruct((2, members), f32),
        ),
        in_specs=[pl.BlockSpec(memory_space=pltpu.HBM)] * 4,
        out_specs=(VMEM, VMEM, VMEM),
        scratch_shapes=[
            pltpu.VMEM(own.shape, bf16),
            pltpu.VMEM((8, count), f32),
            pltpu.VMEM((1, count), jnp.int32),
            pltpu.VMEM((SIDE_Z, SIDE_Y, seats, rows, size), bf16),
            pltpu.VMEM((SIDE_Z, SIDE_Y, seats * rows, size), bf16),
            pltpu.VMEM((SIDE_Z + 1, 8, watches), f32),
            pltpu.VMEM((size, watches), bf16),
            pltpu.VMEM((SIDE_Z + 1, SIDE_Y, seats * rows, watches), bf16),
            pltpu.VMEM((CORES, packed, TILE), f32),
            pltpu.VMEM((packed, TILE), f32),
            pltpu.VMEM((SIDE_X * SIDE_Y, part, TILE), f32),
            pltpu.VMEM((PLANE + 1, 2, members), f32),
            pltpu.VMEM((packed, TILE), f32),
            pltpu.SemaphoreType.DMA((4,)),
            pltpu.SemaphoreType.DMA((9,)),
            pltpu.SemaphoreType.DMA((9,)),
            pltpu.SemaphoreType.DMA((SIDE_Z,)),
            pltpu.SemaphoreType.DMA((SIDE_X * SIDE_Y,)),
        ],
        compiler_params=pltpu.CompilerParams(
            collective_id=0, has_side_effects=True, vmem_limit_bytes=ROOM
        ),
    )(*(pltpu.with_memory_space_constraint(a, pltpu.HBM) for a in (own, offsets, observed, variances)))


def scattered(high, low, state, own_rows):
    rows, size = state.shape
    cut = size // 2
    chips, seats = SIDE_X * SIDE_Y, CORES * SIDE_X
    return pl.pallas_call(
        scatter_kernel,
        name="scatter",
        out_shape=jax.ShapeDtypeStruct((chips, SIDE_Z, CORES, own_rows, size), state.dtype),
        in_specs=[VMEM, VMEM, VMEM],
        out_specs=VMEM,
        scratch_shapes=[
            pltpu.VMEM((SIDE_Y, SIDE_Z, seats, own_rows, size), state.dtype),
            pltpu.VMEM((PLANE, seats, own_rows, cut), state.dtype),
            pltpu.VMEM((SIDE_Z, chips, CORES, own_rows, size - cut), state.dtype),
            pltpu.SemaphoreType.DMA,
            pltpu.SemaphoreType.DMA((SIDE_Z, SIDE_Y)),
            pltpu.SemaphoreType.DMA,
            pltpu.SemaphoreType.DMA,
            pltpu.SemaphoreType.DMA,
            pltpu.SemaphoreType.DMA,
            pltpu.SemaphoreType.DMA,
            pltpu.SemaphoreType.DMA,
        ],
        compiler_params=pltpu.CompilerParams(
            collective_id=1, has_side_effects=True, vmem_limit_bytes=ROOM
        ),
    )(high, low, state)


def split_bf16(a):
    high = a.astype(jnp.bfloat16)
    return high, (a - high.astype(jnp.float32)).astype(jnp.bfloat16)


def dot1(a, b):
    return jnp.dot(
        a.astype(jnp.bfloat16), b.astype(jnp.bfloat16), preferred_element_type=jnp.float32
    )


def dot6(a, b):
    return jnp.dot(a, b, precision=lax.Precision.HIGHEST, preferred_element_type=jnp.float32)


WELL_CONDITIONED = 2000.0
ROUNDING = 1e-6


def by_rows(rows, body, init=None):
    def step(i, carry):
        return body(pl.ds(pl.multiple_of(i * TILE, TILE), TILE), carry)

    return lax.fori_loop(0, rows // TILE, step, init)


def largest_row(m):
    return jnp.max(jnp.sum(jnp.abs(m), axis=1))


def sum_of_squares(m):
    return jnp.sum(m * m)


def unit(rows, n):
    row = lax.broadcasted_iota(jnp.int32, (TILE, n), 0) + rows.start
    col = lax.broadcasted_iota(jnp.int32, (TILE, n), 1)
    return jnp.where(row == col, 1.0, 0.0).astype(jnp.float32)


EXTRA = 16


def residual_squares(left):
    return jnp.sum(jnp.sum(left * left, axis=0, keepdims=True))


def quick_inverse(x, system, r, parts, both):
    n = system.shape[1]
    rows = system.shape[0]

    def passes(lhs, rhs):
        return jnp.dot(lhs, rhs, preferred_element_type=jnp.float32)

    values = system[...]
    high = values.astype(jnp.bfloat16)
    parts[pl.ds(0, rows), :] = high
    parts[pl.ds(rows, rows), :] = (values - high.astype(jnp.float32)).astype(jnp.bfloat16)
    top = pl.ds(0, n)
    r[...] = passes(parts[top, :], parts[top, :])
    bound = jnp.sqrt(jnp.max(jnp.sum(jnp.abs(r[...]), axis=0, keepdims=True)) * 1.02)
    a = 2.0 / (1.0 + bound)

    def first(rows, total):
        eye = unit(rows, n)
        s = system[rows, :] * a
        left = eye - 2.0 * s + (a * a) * r[rows, :]
        grown = a * (2.0 * eye - s)
        x[rows, :] = grown
        both[rows, :] = grown.astype(jnp.bfloat16)
        both[pl.ds(n + rows.start, TILE), :] = left.astype(jnp.bfloat16)
        return total + jnp.sum(left * left, axis=0, keepdims=True)

    total = by_rows(n, first, jnp.zeros((1, n), jnp.float32))

    def more(state):
        count, size = state
        return jnp.logical_and(count < 16, size > 0.01)

    def double(state):
        count, _ = state
        out = passes(both[...], both[pl.ds(n, n), :])
        grown = x[top, :] + out[:n]
        left = out[n:]
        x[top, :] = grown
        both[...] = jnp.concatenate([grown, left]).astype(jnp.bfloat16)
        return count + 1, residual_squares(left)

    lax.while_loop(more, double, (jnp.int32(0), jnp.sum(total)))

    def more_newton(state):
        count, size = state
        return jnp.logical_and(count < 8, size > ROUNDING)

    def newton(state):
        count, _ = state
        now = x[top, :]
        xh = now.astype(jnp.bfloat16)
        xl = (now - xh.astype(jnp.float32)).astype(jnp.bfloat16)
        here_high = parts[pl.ds(0, rows), :]
        out = passes(here_high, xh) + (
            passes(here_high, xl) + passes(parts[pl.ds(rows, rows), :], xh)
        )
        r[...] = out[:n]

        def left_of(at, total):
            left = unit(at, n) - r[at, :]
            both[at, :] = left.astype(jnp.bfloat16)
            return total + jnp.sum(left * left, axis=0, keepdims=True)

        total = by_rows(n, left_of, jnp.zeros((1, n), jnp.float32))
        tail = out[n:]
        grown = jnp.concatenate([now, tail])
        x[...] = grown + passes(jnp.concatenate([xh, tail.astype(jnp.bfloat16)]), both[top, :])
        return count + 1, jnp.sum(total)

    return lax.while_loop(more_newton, newton, (jnp.int32(0), jnp.float32(1.0)))[1]


def careful_inverse(x, system, r, tmp):
    n = system.shape[1]

    def square(rows, bound):
        tmp[rows, :] = dot6(system[rows, :], system[pl.ds(0, n), :])
        return jnp.maximum(bound, largest_row(tmp[rows, :]))

    bound = jnp.sqrt(by_rows(n, square, jnp.float32(0.0)) * 1.02)
    a = 2.0 / (1.0 + bound)

    def first(rows, total):
        eye = unit(rows, n)
        s = system[rows, :] * a
        x[rows, :] = a * (2.0 * eye - s)
        left = eye - 2.0 * s + (a * a) * tmp[rows, :]
        r[rows, :] = left
        return total + sum_of_squares(left)

    def more(state):
        count, size = state
        return jnp.logical_and(count < 40, size > 4e-4)

    def double(state):
        def grow(rows, _):
            x[rows, :] += dot6(x[rows, :], r[...])
            tmp[rows, :] = dot6(r[rows, :], r[...])
            return 0

        by_rows(n, grow, 0)

        def take(rows, total):
            left = tmp[rows, :]
            r[rows, :] = left
            return total + sum_of_squares(left)

        return state[0] + 1, by_rows(n, take, jnp.float32(0.0))

    lax.while_loop(more, double, (jnp.int32(0), by_rows(n, first, jnp.float32(0.0))))

    def more_newton(state):
        count, size = state
        return jnp.logical_and(count < 12, size > ROUNDING)

    def newton(state):
        def residual(rows, total):
            left = unit(rows, n) - dot6(system[rows, :], x[pl.ds(0, n), :])
            r[rows, :] = left
            return total + sum_of_squares(left)

        size = by_rows(n, residual, jnp.float32(0.0))

        def correct(rows, _):
            x[rows, :] += dot6(x[rows, :], r[...])
            return 0

        by_rows(n, correct, 0)
        return state[0] + 1, size

    lax.while_loop(more_newton, newton, (jnp.int32(0), jnp.float32(1.0)))
    last = pl.ds(n, system.shape[0] - n)
    x[last, :] = dot6(system[last, :], x[pl.ds(0, n), :])


def mixing_kernel(products, sums, high, low, x, system, r, parts, both):
    n = sums.shape[1]
    tiles = n // TILE
    square = jnp.sum(sums[1:2, 0:1] / sums[1:2, 1:2])
    inflation = jnp.sqrt(jnp.full((1, n), square, jnp.float32))
    row = lax.broadcasted_iota(jnp.int32, (TILE, TILE), 0)
    col = lax.broadcasted_iota(jnp.int32, (TILE, TILE), 1)
    eye = jnp.where(row == col, 1.0, 0.0).astype(jnp.float32)
    corners = [i * (i + 3) // 2 for i in range(tiles)]
    diagonal = sum(products[block] for block in corners)
    trace = jnp.sum(jnp.sum(eye * diagonal, axis=0, keepdims=True)) * square
    shift = trace / ((n - 1.0) * n)
    block = 0
    for i in range(tiles):
        down = pl.ds(i * TILE, TILE)
        for j in range(i + 1):
            across = pl.ds(j * TILE, TILE)
            values = products[block] * square + shift
            if i == j:
                system[down, down] = values + eye
            else:
                system[down, across] = values
                system[across, down] = values.T
            block += 1

    def longest(rows, most):
        return most + jnp.sum(jnp.abs(system[rows, :]), axis=0, keepdims=True)

    most = jnp.max(by_rows(n, longest, jnp.zeros((1, n), jnp.float32)))
    first = lax.broadcasted_iota(jnp.int32, (EXTRA, n), 0) == 0
    system[pl.ds(n, EXTRA), :] = jnp.where(first, sums[0:1, :], 0.0)
    left = lax.cond(
        most < WELL_CONDITIONED,
        lambda: quick_inverse(x, system, r, parts, both),
        lambda: jnp.float32(1.0),
    )

    @pl.when(jnp.logical_not(left <= ROUNDING))
    def _():
        pl.run_scoped(
            lambda tmp: careful_inverse(x, system, r, tmp), pltpu.VMEM((n, n), jnp.float32)
        )

    q = x[pl.ds(n, 1), :] * square

    def mix(rows, _):
        eye = unit(rows, n)
        mixing = (0.5 * inflation) * (eye + x[rows, :]) + q
        mean = jnp.sum(mixing, axis=1, keepdims=True) * (1.0 / n)
        high[rows, :], low[rows, :] = split_bf16(mixing - mean + 1.0 / n)
        return 0

    by_rows(n, mix, 0)


def mixed(products, sums):
    n = sums.shape[1]
    return pl.pallas_call(
        mixing_kernel,
        name="mixing",
        out_shape=[jax.ShapeDtypeStruct((n, n), jnp.bfloat16)] * 2,
        in_specs=[VMEM, VMEM],
        out_specs=[VMEM, VMEM],
        scratch_shapes=[
            pltpu.VMEM((n + EXTRA, n), jnp.float32),
            pltpu.VMEM((n + EXTRA, n), jnp.float32),
            pltpu.VMEM((n, n), jnp.float32),
            pltpu.VMEM((2 * (n + EXTRA), n), jnp.bfloat16),
            pltpu.VMEM((2 * n, n), jnp.bfloat16),
        ],
        compiler_params=pltpu.CompilerParams(vmem_limit_bytes=ROOM),
    )(products.reshape(-1, TILE, TILE), sums)


def put_out_kernel(own, out, laid, done):
    size = own.shape[2]
    share = own.shape[0] // PARTS

    def part(k):
        return links_of(k, share * size)

    @pl.loop(0, PARTS)
    def _(k):
        for i in range(share):
            laid[:, links_of(k * share + i, size)] = own[k * share + i]

        pltpu.make_async_copy(laid.at[:, part(k)], out.at[:, part(k)], done.at[k]).start()

    @pl.loop(0, PARTS)
    def _(k):
        pltpu.make_async_copy(laid.at[:, part(k)], out.at[:, part(k)], done.at[k]).wait()


PARTS = 8


def put_out(own):
    rows, size = own.shape[-2:]
    own = own.reshape(-1, rows, size)
    shape = (rows, len(own) * size)
    return pl.pallas_call(
        put_out_kernel,
        name="put_out",
        out_shape=jax.ShapeDtypeStruct(shape, own.dtype),
        in_specs=[VMEM],
        out_specs=pl.BlockSpec(memory_space=pltpu.HBM),
        scratch_shapes=[pltpu.VMEM(shape, own.dtype), pltpu.SemaphoreType.DMA((PARTS,))],
        compiler_params=pltpu.CompilerParams(vmem_limit_bytes=ROOM),
    )(own)


def local(ensemble, obs_offset, observed, obs_var):
    state, products, sums = gathered(ensemble, obs_offset, observed, obs_var)
    high, low = mixed(products, sums)
    return put_out(scattered(high, low, state.reshape(sums.shape[1], -1), len(ensemble)))


def solution(mesh):
    finer = Mesh(
        mesh.devices.reshape(4, 8, 2, mesh.shape["region"]),
        ("member_0", "member_1", "member_2", "region"),
    )
    in_specs = (
        P(MEMBER_REGION, None),
        P("region", MEMBER, None),
        P("region", MEMBER, None),
        P("region", MEMBER, None),
    )
    out_specs = P(MEMBER_REGION, None)
    return jax.shard_map(local, mesh=finer, in_specs=in_specs, out_specs=out_specs, check_vma=False)
```

```python
import jax
import jax.numpy as jnp
from jax import lax
from jax.experimental import pallas as pl
from jax.experimental.pallas import tpu as pltpu
from jax.sharding import Mesh
from jax.sharding import PartitionSpec as P

MEMBER = ("member_0", "member_1", "member_2")
MEMBER_REGION = ("member_0", "member_1", "member_2", "region")


MESH_ID = pl.DeviceIdType.MESH
SIDE_Y, SIDE_Z, CORES, SIDE_X = 4, 8, 2, 4
TILE = 128


def here():
    return (
        lax.axis_index("region"),
        lax.axis_index("member_0"),
        lax.axis_index("member_1"),
        lax.axis_index("member_2"),
    )


def device(x, y, z, c):
    return (y, z, c, x)


def chip_peer(i):
    x, y, z, c = here()
    i = lax.rem(i * 7, SIDE_X * SIDE_Y)
    return lax.rem(x + i, SIDE_X), lax.rem(y + i // SIDE_X, SIDE_Y), z, c


def in_plane(i):
    return lax.rem(i // 4, 4), lax.rem(i // 16, 2), lax.rem(i, 4)


PLANE = SIDE_X * SIDE_Y * CORES


def plane_peer(i):
    x, y, z, c = here()
    dy, dc, dx = in_plane(lax.rem(i * 13, PLANE))
    return lax.rem(x + dx, SIDE_X), lax.rem(y + dy, SIDE_Y), z, lax.rem(c + dc, CORES)


def line_peer(i):
    x, y, z, c = here()
    return x, y, lax.rem(z + i, SIDE_Z), c


def greet(barrier):
    @pl.loop(1, PLANE)
    def _(i):
        pl.semaphore_signal(barrier, 1, device_id=device(*plane_peer(i)), device_id_type=MESH_ID)

    @pl.loop(1, SIDE_Z)
    def _(i):
        pl.semaphore_signal(barrier, 1, device_id=device(*line_peer(i)), device_id_type=MESH_ID)


def met(barrier):
    pl.semaphore_wait(barrier, PLANE - 1 + SIDE_Z - 1)


def remote(src, dst, send, recv, place):
    return pltpu.make_async_remote_copy(
        src, dst, send, recv, device_id=device(*place), device_id_type=MESH_ID
    )


def block_of(x, y, z, c):
    return ((x * SIDE_Y + y) * SIDE_Z + z) * CORES + c


def links_of(block, size):
    return pl.ds(pl.multiple_of(block * size, size), size)


def no_matter(ref, send, recv):
    return remote(ref, ref, send, recv, here())


def dot6_t(a, b):
    return lax.dot_general(
        a,
        b,
        (((1,), (1,)), ((), ())),
        precision=lax.Precision.HIGHEST,
        preferred_element_type=jnp.float32,
    )


def along(k):
    d = k // 2 + 1
    return lax.rem(jnp.where(lax.rem(k, 2) == 0, d, SIDE_Z - d), SIDE_Z) * jnp.where(k == 7, 0, 1)


EARLY = 2
HALVES = 2
HALFWAY = 4


def gather_kernel(
    ensemble, offsets, observed, variances, whole, total, sums,
    own, notes, numbers, pieces, stage, all_notes, seen, picked, half, chunks, extras,
    twin, tables, anomalies, weighted, copied, send, recv, arrived, parted,
):
    x, y, z, c = here()
    size = own.shape[1] // (PLANE * SIDE_Z)
    members = sums.shape[1]
    seat = c * SIDE_X + x
    loads = [
        pltpu.make_async_copy(ensemble, own, copied.at[0]),
        pltpu.make_async_copy(offsets.at[0], numbers, copied.at[1]),
        pltpu.make_async_copy(observed.at[0], notes.at[pl.ds(1, 1), :], copied.at[2]),
        pltpu.make_async_copy(variances.at[0], notes.at[pl.ds(2, 1), :], copied.at[3]),
    ]
    for load in loads:
        load.start()
    barrier = pltpu.get_barrier_semaphore()
    greet(barrier)
    for load in loads:
        load.wait()
    notes[0:1, :] = numbers[...].astype(jnp.float32)
    count, watches = notes.shape[1], all_notes.shape[2]
    to = lax.broadcasted_iota(jnp.int32, (count, watches), 1)
    at = lax.broadcasted_iota(jnp.int32, (count, watches), 0) + z * count
    row = lax.broadcasted_iota(jnp.int32, (8, count), 0)
    placed = dot6(
        jnp.where(row < 3, notes[...], 0.0), jnp.where(to == at, 1.0, 0.0).astype(jnp.float32)
    )
    mine = all_notes.at[SIDE_Z]
    mine[...] = placed

    @pl.loop(0, SIDE_Z)
    def _(t):
        pieces[t, y, seat] = own[:, links_of(block_of(x, y, t, c), size)]

    met(barrier)

    @pl.loop(1, SIDE_Z)
    def _(i):
        remote(mine, all_notes.at[z], send.at[0], recv.at[0], line_peer(i)).start()

    @pl.loop(0, SIDE_Z)
    def _(k):
        t = lax.rem(z + along(k), SIDE_Z)

        @pl.loop(1, PLANE)
        def _(i):
            px, py, _, pc = plane_peer(i)
            remote(
                own.at[:, links_of(block_of(px, py, t, pc), size)],
                pieces.at[t, y, seat],
                send.at[1],
                arrived.at[t],
                (px, py, z, pc),
            ).start()

    all_notes[z] = placed
    no_matter(all_notes.at[pl.ds(0, SIDE_Z - 1)], send.at[0], recv.at[0]).wait()
    table = jnp.sum(all_notes[pl.ds(0, SIDE_Z)], axis=0)
    offset = table[0:1, :].astype(jnp.int32)
    tables[c] = table
    remote(tables.at[c], tables.at[c], send.at[9], recv.at[9], (x, y, z, 1 - c)).start()
    link = lax.broadcasted_iota(jnp.int32, (size, watches), 0)
    seen[...] = jnp.where(link == offset, 1.0, 0.0).astype(jnp.bfloat16)
    line = lax.broadcasted_iota(jnp.int32, (members // SIDE_Z, watches), 1) // count

    def pass_on(k, part):
        t = lax.rem(z + along(k), SIDE_Z)
        some = pl.ds(part * (SIDE_Y // 2), SIDE_Y // 2)
        remote(
            stage.at[t, some], whole.at[some, z], send.at[3], recv.at[3], (x, y, t, c)
        ).start()

    def pick(k, found):
        t = lax.rem(z + along(k), SIDE_Z)
        no_matter(
            own.at[:, pl.ds(0, (PLANE - 1) * size)], send.at[1], arrived.at[t]
        ).wait_recv()

        def lay(j, _):
            stage[t, j] = pieces[t, j].reshape(stage.shape[2:])
            return 0

        lax.fori_loop(0, SIDE_Y, lay, 0)
        rows = stage[t].reshape(members // SIDE_Z, size)
        values = jnp.dot(rows, seen[...], preferred_element_type=jnp.float32)

        @pl.when(jnp.logical_and(k >= 1, k <= EARLY + HALVES))
        def _():
            pass_on(k - 1, 0)

        @pl.when(jnp.logical_and(k >= 1, k <= EARLY))
        def _():
            pass_on(k - 1, 1)

        return jnp.where(line == t, values, found)

    found = lax.fori_loop(0, SIDE_Z, pick, jnp.zeros(line.shape, jnp.float32))
    mine = picked.at[SIDE_Z]
    mine[...] = found.astype(jnp.bfloat16).reshape(mine.shape)

    @pl.loop(1, SIDE_Z)
    def _(i):
        remote(mine, picked.at[z], send.at[2], recv.at[2], line_peer(i)).start()

    @pl.loop(EARLY, EARLY + HALVES)
    def _(k):
        pass_on(k, 1)

    @pl.loop(EARLY + HALVES, SIDE_Z - 1)
    def _(k):
        pass_on(k, 0)
        pass_on(k, 1)

    picked[z] = mine[...]
    whole[:, z] = stage[z]
    no_matter(
        own.at[:, pl.ds(0, (PLANE - 1) * SIDE_Z * size)], send.at[1], recv.at[1]
    ).wait_send()
    no_matter(picked.at[pl.ds(0, SIDE_Z - 1)], send.at[2], recv.at[2]).wait()

    partner = (x, y, z, 1 - c)
    near = picked.at[pl.ds(0, SIDE_Z)]
    remote(near, twin, send.at[4], recv.at[4], partner).start()

    def terms(found, facts, core):
        measured, variance = facts[1:2, :], facts[2:3, :]
        values = jnp.swapaxes(found, 0, 1).reshape(members, watches).astype(jnp.float32)
        center = jnp.sum(values, axis=0, keepdims=True) * (1.0 / members)
        anomaly = values - center
        innovation = measured - center
        weight = 1.0 / ((members - 1.0) * variance)
        at = links_of(core, watches)
        anomalies[:, at] = anomaly
        weighted[:, at] = anomaly * weight
        return anomaly, innovation, weight, variance

    anomaly, innovation, weight, variance = terms(picked[pl.ds(0, SIDE_Z)], table, c)
    spread = jnp.sum(anomaly * anomaly, axis=0, keepdims=True) * (1.0 / (members - 1.0)) + variance
    column = dot6_t(weight * innovation, anomaly)
    numer = jnp.sum(innovation * innovation, axis=1, keepdims=True)
    denom = jnp.sum(spread, axis=1, keepdims=True)
    lane = lax.broadcasted_iota(jnp.int32, column.shape, 1)
    extra = extras.at[PLANE]
    extra[0:1, :] = column
    extra[1:2, :] = jnp.where(lane == 0, numer, jnp.where(lane == 1, denom, 0.0))

    @pl.loop(1, PLANE)
    def _(i):
        remote(
            extra, extras.at[y * (CORES * SIDE_X) + seat], send.at[5], recv.at[5], plane_peer(i)
        ).start()

    extras[y * (CORES * SIDE_X) + seat] = extra[...]
    no_matter(tables.at[0], send.at[9], recv.at[9]).wait()
    no_matter(twin, send.at[4], recv.at[4]).wait()
    terms(twin[...], tables[1 - c], 1 - c)

    tiles = members // TILE
    blocks = [(i, j) for i in range(tiles) for j in range(i + 1)]
    rows = half.shape[0]
    count = rows // TILE
    for k in range(count):
        (i0, j0), (i1, j1) = blocks[k], blocks[count + k]
        i, j = jnp.where(c == 0, i0, i1), jnp.where(c == 0, j0, j1)
        half[k * TILE : (k + 1) * TILE, :] = dot6_t(
            weighted[links_of(i, TILE), :], anomalies[links_of(j, TILE), :]
        )

    chips = SIDE_X * SIDE_Y
    part = rows // chips

    def part_of(px, py):
        return pl.ds(pl.multiple_of((py * SIDE_X + px) * part, part), part)

    @pl.loop(1, chips)
    def _(i):
        place = chip_peer(i)
        remote(
            half.at[part_of(place[0], place[1])],
            chunks.at[y * SIDE_X + x],
            send.at[6],
            recv.at[6],
            place,
        ).start()

    chunks[y * SIDE_X + x] = half[part_of(x, y), :]
    no_matter(chunks.at[pl.ds(0, chips - 1)], send.at[6], recv.at[6]).wait()
    done = total.at[c, part_of(x, y)]
    done[...] = jnp.sum(chunks[...], axis=0)

    @pl.loop(1, chips)
    def _(i):
        place = chip_peer(i)
        remote(done, done, send.at[7], parted.at[y * SIDE_X + x], place).start()

    remote(done, done, send.at[8], recv.at[8], partner).start()

    @pl.loop(1, chips)
    def _(i):
        px, py, _, _ = chip_peer(chips - i)
        piece = total.at[c, part_of(px, py)]
        no_matter(piece, send.at[7], parted.at[py * SIDE_X + px]).wait_recv()
        remote(piece, piece, send.at[8], recv.at[8], partner).start()

    no_matter(half.at[pl.ds(0, rows - part)], send.at[7], recv.at[7]).wait_send()
    no_matter(extras.at[pl.ds(0, PLANE - 1)], send.at[5], recv.at[5]).wait()
    sums[...] = jnp.sum(extras[pl.ds(0, PLANE)], axis=0)
    no_matter(half, send.at[8], recv.at[8]).wait()
    no_matter(stage.at[pl.ds(0, SIDE_Z - 1)], send.at[3], recv.at[3]).wait()


def scatter_kernel(
    high, low, state, own, whole, far, near, send_far, arrived, send_near, recv_near,
    send_last, recv_last, send_own, recv_own,
):
    x, y, z, c = here()
    rows, size = state.shape
    chip, seat = x * SIDE_Y + y, c * SIDE_X + x
    cut = far.shape[-1]
    first, second = pl.ds(0, cut), pl.ds(cut, size - cut)
    barrier = pltpu.get_barrier_semaphore()
    greet(barrier)
    wide = 256


    def analyse(k):
        at = links_of(k, wide)
        values = dot1(high[...], state[:, at]) + dot1(low[...], state[:, at])
        whole[:, :, :, :, at] = values.astype(jnp.bfloat16).reshape(*whole.shape[:-1], wide)

    pl.loop(0, size // wide)(analyse)
    met(barrier)

    @pl.loop(0, SIDE_Z - 1)
    def _(k):
        t = lax.rem(z + along(k), SIDE_Z)

        @pl.loop(0, SIDE_Y)
        def _(dy):
            py = lax.rem(y + dy, SIDE_Y)
            remote(
                whole.at[py, t, :, :, first],
                far.at[z * SIDE_Y + py],
                send_far,
                arrived.at[z, py],
                (x, y, t, c),
            ).start()

    @pl.loop(1, PLANE)
    def _(i):
        px, py, _, pc = plane_peer(i)
        remote(
            whole.at[py, :, pc * SIDE_X + px, :, second],
            near.at[:, chip, c],
            send_near,
            recv_near,
            (px, py, z, pc),
        ).start()

    def hand_on(source, py, dy, t):
        @pl.loop(jnp.where(dy == 0, 1, 0), CORES * SIDE_X)
        def _(j):
            px = lax.rem(x + lax.rem(j, SIDE_X), SIDE_X)
            pc = lax.rem(c + j // SIDE_X, CORES)
            remote(
                source(pc * SIDE_X + px),
                own.at[chip, t, c, :, first],
                send_last,
                recv_last,
                (px, py, z, pc),
            ).start()

        @pl.when(dy == 0)
        def _():
            own[chip, t, c, :, first] = source(seat)[...]

    @pl.loop(0, SIDE_Y)
    def _(dy):
        py = lax.rem(y + dy, SIDE_Y)
        hand_on(lambda s: whole.at[py, z, s, :, first], py, dy, z)

    @pl.loop(0, SIDE_Z)
    def _(t):
        near[t, chip, c] = whole[y, t, seat, :, second]

    def take(k):
        t = lax.rem(z + SIDE_Z - along(k), SIDE_Z)

        @pl.loop(0, SIDE_Y)
        def _(dy):
            py = lax.rem(y + dy, SIDE_Y)
            no_matter(far.at[t * SIDE_Y + py], send_far, arrived.at[t, py]).wait_recv()
            hand_on(lambda s: far.at[t * SIDE_Y + py, s], py, dy, t)

    pl.loop(0, HALFWAY)(take)
    chips = SIDE_X * SIDE_Y
    others = far.at[pl.ds(0, PLANE - 1)]
    no_matter(others, send_near, recv_near).wait()

    @pl.loop(0, SIDE_Z - 1)
    def _(k):
        t = lax.rem(z + along(k), SIDE_Z)
        remote(
            near.at[t], own.at[:, z, :, :, second], send_own, recv_own, (x, y, t, c)
        ).start()

    @pl.loop(0, chips)
    def _(i):
        own[i, z, :, :, second] = near[z, i]

    pl.loop(HALFWAY, SIDE_Z - 1)(take)
    no_matter(far.at[pl.ds(0, (SIDE_Z - 1) * SIDE_Y)], send_far, recv_near).wait_send()
    no_matter(near.at[pl.ds(0, SIDE_Z - 1)], send_own, recv_own).wait()
    no_matter(others, send_last, recv_last).wait()


VMEM = pl.BlockSpec(memory_space=pltpu.VMEM)
ROOM = 24 << 20


def gathered(own, offsets, observed, variances):
    rows = own.shape[0]
    size = own.shape[1] // (PLANE * SIDE_Z)
    members = rows * PLANE * SIDE_Z
    seats = CORES * SIDE_X
    count = offsets.shape[-1]
    watches = SIDE_Z * count
    tiles = members // TILE
    packed = tiles * (tiles + 1) // 2 * TILE // CORES
    part = packed // (SIDE_X * SIDE_Y)
    f32, bf16 = jnp.float32, jnp.bfloat16
    return pl.pallas_call(
        gather_kernel,
        name="gather",
        out_shape=(
            jax.ShapeDtypeStruct((SIDE_Y, SIDE_Z, seats * rows, size), bf16),
            jax.ShapeDtypeStruct((CORES, packed, TILE), f32),
            jax.ShapeDtypeStruct((2, members), f32),
        ),
        in_specs=[pl.BlockSpec(memory_space=pltpu.HBM)] * 4,
        out_specs=(VMEM, VMEM, VMEM),
        scratch_shapes=[
            pltpu.VMEM(own.shape, bf16),
            pltpu.VMEM((8, count), f32),
            pltpu.VMEM((1, count), jnp.int32),
            pltpu.VMEM((SIDE_Z, SIDE_Y, seats, rows, size), bf16),
            pltpu.VMEM((SIDE_Z, SIDE_Y, seats * rows, size), bf16),
            pltpu.VMEM((SIDE_Z + 1, 8, watches), f32),
            pltpu.VMEM((size, watches), bf16),
            pltpu.VMEM((SIDE_Z + 1, SIDE_Y, seats * rows, watches), bf16),
            pltpu.VMEM((packed, TILE), f32),
            pltpu.VMEM((SIDE_X * SIDE_Y, part, TILE), f32),
            pltpu.VMEM((PLANE + 1, 2, members), f32),
            pltpu.VMEM((SIDE_Z, SIDE_Y, seats * rows, watches), bf16),
            pltpu.VMEM((CORES, 8, watches), f32),
            pltpu.VMEM((members, CORES * watches), f32),
            pltpu.VMEM((members, CORES * watches), f32),
            pltpu.SemaphoreType.DMA((4,)),
            pltpu.SemaphoreType.DMA((10,)),
            pltpu.SemaphoreType.DMA((10,)),
            pltpu.SemaphoreType.DMA((SIDE_Z,)),
            pltpu.SemaphoreType.DMA((SIDE_X * SIDE_Y,)),
        ],
        compiler_params=pltpu.CompilerParams(
            collective_id=0, has_side_effects=True, vmem_limit_bytes=ROOM
        ),
    )(*(pltpu.with_memory_space_constraint(a, pltpu.HBM) for a in (own, offsets, observed, variances)))


def scattered(high, low, state, own_rows):
    rows, size = state.shape
    cut = size // 2
    chips, seats = SIDE_X * SIDE_Y, CORES * SIDE_X
    return pl.pallas_call(
        scatter_kernel,
        name="scatter",
        out_shape=jax.ShapeDtypeStruct((chips, SIDE_Z, CORES, own_rows, size), state.dtype),
        in_specs=[VMEM, VMEM, VMEM],
        out_specs=VMEM,
        scratch_shapes=[
            pltpu.VMEM((SIDE_Y, SIDE_Z, seats, own_rows, size), state.dtype),
            pltpu.VMEM((PLANE, seats, own_rows, cut), state.dtype),
            pltpu.VMEM((SIDE_Z, chips, CORES, own_rows, size - cut), state.dtype),
            pltpu.SemaphoreType.DMA,
            pltpu.SemaphoreType.DMA((SIDE_Z, SIDE_Y)),
            pltpu.SemaphoreType.DMA,
            pltpu.SemaphoreType.DMA,
            pltpu.SemaphoreType.DMA,
            pltpu.SemaphoreType.DMA,
            pltpu.SemaphoreType.DMA,
            pltpu.SemaphoreType.DMA,
        ],
        compiler_params=pltpu.CompilerParams(
            collective_id=1, has_side_effects=True, vmem_limit_bytes=ROOM
        ),
    )(high, low, state)


def split_bf16(a):
    high = a.astype(jnp.bfloat16)
    return high, (a - high.astype(jnp.float32)).astype(jnp.bfloat16)


def dot1(a, b):
    return jnp.dot(
        a.astype(jnp.bfloat16), b.astype(jnp.bfloat16), preferred_element_type=jnp.float32
    )


def dot6(a, b):
    return jnp.dot(a, b, precision=lax.Precision.HIGHEST, preferred_element_type=jnp.float32)


WELL_CONDITIONED = 2000.0
ROUNDING = 1e-6


def by_rows(rows, body, init=None):
    def step(i, carry):
        return body(pl.ds(pl.multiple_of(i * TILE, TILE), TILE), carry)

    return lax.fori_loop(0, rows // TILE, step, init)


def largest_row(m):
    return jnp.max(jnp.sum(jnp.abs(m), axis=1))


def sum_of_squares(m):
    return jnp.sum(m * m)


def unit(rows, n):
    row = lax.broadcasted_iota(jnp.int32, (TILE, n), 0) + rows.start
    col = lax.broadcasted_iota(jnp.int32, (TILE, n), 1)
    return jnp.where(row == col, 1.0, 0.0).astype(jnp.float32)


EXTRA = 16


def residual_squares(left):
    return jnp.sum(jnp.sum(left * left, axis=0, keepdims=True))


def quick_inverse(x, system, r, parts, both):
    n = system.shape[1]
    rows = system.shape[0]

    def passes(lhs, rhs):
        return jnp.dot(lhs, rhs, preferred_element_type=jnp.float32)

    values = system[...]
    high = values.astype(jnp.bfloat16)
    parts[pl.ds(0, rows), :] = high
    parts[pl.ds(rows, rows), :] = (values - high.astype(jnp.float32)).astype(jnp.bfloat16)
    top = pl.ds(0, n)
    r[...] = passes(parts[top, :], parts[top, :])
    square = r[...].astype(jnp.bfloat16)
    fourth = jnp.max(jnp.sum(jnp.abs(passes(square, square)), axis=0, keepdims=True))
    bound = jnp.sqrt(jnp.sqrt(fourth * 1.05))
    a = 2.0 / (1.0 + bound)

    def first(rows, total):
        eye = unit(rows, n)
        s = system[rows, :] * a
        left = eye - 2.0 * s + (a * a) * r[rows, :]
        grown = a * (2.0 * eye - s)
        x[rows, :] = grown
        both[rows, :] = grown.astype(jnp.bfloat16)
        both[pl.ds(n + rows.start, TILE), :] = left.astype(jnp.bfloat16)
        return total + jnp.sum(left * left, axis=0, keepdims=True)

    total = by_rows(n, first, jnp.zeros((1, n), jnp.float32))

    def more(state):
        count, size = state
        return jnp.logical_and(count < 16, size > 0.01)

    def double(state):
        count, _ = state
        out = passes(both[...], both[pl.ds(n, n), :])
        grown = x[top, :] + out[:n]
        left = out[n:]
        x[top, :] = grown
        both[...] = jnp.concatenate([grown, left]).astype(jnp.bfloat16)
        return count + 1, residual_squares(left)

    lax.while_loop(more, double, (jnp.int32(0), jnp.sum(total)))

    def more_newton(state):
        count, size = state
        return jnp.logical_and(count < 8, size > ROUNDING)

    def newton(state):
        count, _ = state
        now = x[top, :]
        xh = now.astype(jnp.bfloat16)
        xl = (now - xh.astype(jnp.float32)).astype(jnp.bfloat16)
        here_high = parts[pl.ds(0, rows), :]
        out = passes(here_high, xh) + (
            passes(here_high, xl) + passes(parts[pl.ds(rows, rows), :], xh)
        )
        r[...] = out[:n]

        def left_of(at, total):
            left = unit(at, n) - r[at, :]
            both[at, :] = left.astype(jnp.bfloat16)
            return total + jnp.sum(left * left, axis=0, keepdims=True)

        total = by_rows(n, left_of, jnp.zeros((1, n), jnp.float32))
        tail = out[n:]
        grown = jnp.concatenate([now, tail])
        x[...] = grown + passes(jnp.concatenate([xh, tail.astype(jnp.bfloat16)]), both[top, :])
        return count + 1, jnp.sum(total)

    return lax.while_loop(more_newton, newton, (jnp.int32(0), jnp.float32(1.0)))[1]


def careful_inverse(x, system, r, tmp):
    n = system.shape[1]

    def square(rows, bound):
        tmp[rows, :] = dot6(system[rows, :], system[pl.ds(0, n), :])
        return jnp.maximum(bound, largest_row(tmp[rows, :]))

    bound = jnp.sqrt(by_rows(n, square, jnp.float32(0.0)) * 1.02)
    a = 2.0 / (1.0 + bound)

    def first(rows, total):
        eye = unit(rows, n)
        s = system[rows, :] * a
        x[rows, :] = a * (2.0 * eye - s)
        left = eye - 2.0 * s + (a * a) * tmp[rows, :]
        r[rows, :] = left
        return total + sum_of_squares(left)

    def more(state):
        count, size = state
        return jnp.logical_and(count < 40, size > 4e-4)

    def double(state):
        def grow(rows, _):
            x[rows, :] += dot6(x[rows, :], r[...])
            tmp[rows, :] = dot6(r[rows, :], r[...])
            return 0

        by_rows(n, grow, 0)

        def take(rows, total):
            left = tmp[rows, :]
            r[rows, :] = left
            return total + sum_of_squares(left)

        return state[0] + 1, by_rows(n, take, jnp.float32(0.0))

    lax.while_loop(more, double, (jnp.int32(0), by_rows(n, first, jnp.float32(0.0))))

    def more_newton(state):
        count, size = state
        return jnp.logical_and(count < 12, size > ROUNDING)

    def newton(state):
        def residual(rows, total):
            left = unit(rows, n) - dot6(system[rows, :], x[pl.ds(0, n), :])
            r[rows, :] = left
            return total + sum_of_squares(left)

        size = by_rows(n, residual, jnp.float32(0.0))

        def correct(rows, _):
            x[rows, :] += dot6(x[rows, :], r[...])
            return 0

        by_rows(n, correct, 0)
        return state[0] + 1, size

    lax.while_loop(more_newton, newton, (jnp.int32(0), jnp.float32(1.0)))
    last = pl.ds(n, system.shape[0] - n)
    x[last, :] = dot6(system[last, :], x[pl.ds(0, n), :])


def mixing_kernel(products, sums, high, low, x, system, r, parts, both):
    n = sums.shape[1]
    tiles = n // TILE
    square = jnp.sum(sums[1:2, 0:1] / sums[1:2, 1:2])
    inflation = jnp.sqrt(jnp.full((1, n), square, jnp.float32))
    row = lax.broadcasted_iota(jnp.int32, (TILE, TILE), 0)
    col = lax.broadcasted_iota(jnp.int32, (TILE, TILE), 1)
    eye = jnp.where(row == col, 1.0, 0.0).astype(jnp.float32)
    corners = [i * (i + 3) // 2 for i in range(tiles)]
    diagonal = sum(products[block] for block in corners)
    trace = jnp.sum(jnp.sum(eye * diagonal, axis=0, keepdims=True)) * square
    shift = trace / ((n - 1.0) * n)
    block = 0
    for i in range(tiles):
        down = pl.ds(i * TILE, TILE)
        for j in range(i + 1):
            across = pl.ds(j * TILE, TILE)
            values = products[block] * square + shift
            if i == j:
                system[down, down] = values + eye
            else:
                system[down, across] = values
                system[across, down] = values.T
            block += 1

    def longest(rows, most):
        return most + jnp.sum(jnp.abs(system[rows, :]), axis=0, keepdims=True)

    most = jnp.max(by_rows(n, longest, jnp.zeros((1, n), jnp.float32)))
    first = lax.broadcasted_iota(jnp.int32, (EXTRA, n), 0) == 0
    system[pl.ds(n, EXTRA), :] = jnp.where(first, sums[0:1, :], 0.0)
    left = lax.cond(
        most < WELL_CONDITIONED,
        lambda: quick_inverse(x, system, r, parts, both),
        lambda: jnp.float32(1.0),
    )

    @pl.when(jnp.logical_not(left <= ROUNDING))
    def _():
        pl.run_scoped(
            lambda tmp: careful_inverse(x, system, r, tmp), pltpu.VMEM((n, n), jnp.float32)
        )

    q = x[pl.ds(n, 1), :] * square

    def mix(rows, _):
        eye = unit(rows, n)
        mixing = (0.5 * inflation) * (eye + x[rows, :]) + q
        mean = jnp.sum(mixing, axis=1, keepdims=True) * (1.0 / n)
        high[rows, :], low[rows, :] = split_bf16(mixing - mean + 1.0 / n)
        return 0

    by_rows(n, mix, 0)


def mixed(products, sums):
    n = sums.shape[1]
    return pl.pallas_call(
        mixing_kernel,
        name="mixing",
        out_shape=[jax.ShapeDtypeStruct((n, n), jnp.bfloat16)] * 2,
        in_specs=[VMEM, VMEM],
        out_specs=[VMEM, VMEM],
        scratch_shapes=[
            pltpu.VMEM((n + EXTRA, n), jnp.float32),
            pltpu.VMEM((n + EXTRA, n), jnp.float32),
            pltpu.VMEM((n, n), jnp.float32),
            pltpu.VMEM((2 * (n + EXTRA), n), jnp.bfloat16),
            pltpu.VMEM((2 * n, n), jnp.bfloat16),
        ],
        compiler_params=pltpu.CompilerParams(vmem_limit_bytes=ROOM),
    )(products.reshape(-1, TILE, TILE), sums)


def put_out_kernel(own, out, laid, done):
    size = own.shape[2]
    share = own.shape[0] // PARTS

    def part(k):
        return links_of(k, share * size)

    @pl.loop(0, PARTS)
    def _(k):
        for i in range(share):
            laid[:, links_of(k * share + i, size)] = own[k * share + i]

        pltpu.make_async_copy(laid.at[:, part(k)], out.at[:, part(k)], done.at[k]).start()

    @pl.loop(0, PARTS)
    def _(k):
        pltpu.make_async_copy(laid.at[:, part(k)], out.at[:, part(k)], done.at[k]).wait()


PARTS = 8


def put_out(own):
    rows, size = own.shape[-2:]
    own = own.reshape(-1, rows, size)
    shape = (rows, len(own) * size)
    return pl.pallas_call(
        put_out_kernel,
        name="put_out",
        out_shape=jax.ShapeDtypeStruct(shape, own.dtype),
        in_specs=[VMEM],
        out_specs=pl.BlockSpec(memory_space=pltpu.HBM),
        scratch_shapes=[pltpu.VMEM(shape, own.dtype), pltpu.SemaphoreType.DMA((PARTS,))],
        compiler_params=pltpu.CompilerParams(vmem_limit_bytes=ROOM),
    )(own)


def local(ensemble, obs_offset, observed, obs_var):
    state, products, sums = gathered(ensemble, obs_offset, observed, obs_var)
    high, low = mixed(products, sums)
    return put_out(scattered(high, low, state.reshape(sums.shape[1], -1), len(ensemble)))


def solution(mesh):
    finer = Mesh(
        mesh.devices.reshape(4, 8, 2, mesh.shape["region"]),
        ("member_0", "member_1", "member_2", "region"),
    )
    in_specs = (
        P(MEMBER_REGION, None),
        P("region", MEMBER, None),
        P("region", MEMBER, None),
        P("region", MEMBER, None),
    )
    out_specs = P(MEMBER_REGION, None)
    return jax.shard_map(local, mesh=finer, in_specs=in_specs, out_specs=out_specs, check_vma=False)
```

```python
import jax
import jax.numpy as jnp
from jax import lax
from jax.experimental import pallas as pl
from jax.experimental.pallas import tpu as pltpu
from jax.sharding import Mesh
from jax.sharding import PartitionSpec as P

MEMBER = ("member_0", "member_1", "member_2")
MEMBER_REGION = ("member_0", "member_1", "member_2", "region")


MESH_ID = pl.DeviceIdType.MESH
SIDE_Y, SIDE_Z, CORES, SIDE_X = 4, 8, 2, 4
TILE = 128


def here():
    return (
        lax.axis_index("region"),
        lax.axis_index("member_0"),
        lax.axis_index("member_1"),
        lax.axis_index("member_2"),
    )


def device(x, y, z, c):
    return (y, z, c, x)


def chip_peer(i):
    x, y, z, c = here()
    i = lax.rem(i * 7, SIDE_X * SIDE_Y)
    return lax.rem(x + i, SIDE_X), lax.rem(y + i // SIDE_X, SIDE_Y), z, c


def in_plane(i):
    return lax.rem(i // 4, 4), lax.rem(i // 16, 2), lax.rem(i, 4)


PLANE = SIDE_X * SIDE_Y * CORES


def plane_peer(i):
    x, y, z, c = here()
    dy, dc, dx = in_plane(lax.rem(i * 13, PLANE))
    return lax.rem(x + dx, SIDE_X), lax.rem(y + dy, SIDE_Y), z, lax.rem(c + dc, CORES)


def line_peer(i):
    x, y, z, c = here()
    return x, y, lax.rem(z + i, SIDE_Z), c


def greet(barrier):
    @pl.loop(1, PLANE)
    def _(i):
        pl.semaphore_signal(barrier, 1, device_id=device(*plane_peer(i)), device_id_type=MESH_ID)

    @pl.loop(1, SIDE_Z)
    def _(i):
        pl.semaphore_signal(barrier, 1, device_id=device(*line_peer(i)), device_id_type=MESH_ID)


def met(barrier):
    pl.semaphore_wait(barrier, PLANE - 1 + SIDE_Z - 1)


def remote(src, dst, send, recv, place):
    return pltpu.make_async_remote_copy(
        src, dst, send, recv, device_id=device(*place), device_id_type=MESH_ID
    )


def block_of(x, y, z, c):
    return ((x * SIDE_Y + y) * SIDE_Z + z) * CORES + c


def links_of(block, size):
    return pl.ds(pl.multiple_of(block * size, size), size)


def no_matter(ref, send, recv):
    return remote(ref, ref, send, recv, here())


def dot6_t(a, b):
    return lax.dot_general(
        a,
        b,
        (((1,), (1,)), ((), ())),
        precision=lax.Precision.HIGHEST,
        preferred_element_type=jnp.float32,
    )


def along(k):
    d = k // 2 + 1
    return lax.rem(jnp.where(lax.rem(k, 2) == 0, d, SIDE_Z - d), SIDE_Z) * jnp.where(k == 7, 0, 1)


EARLY = 2
HALVES = 2
HALFWAY = 4


def gather_kernel(
    ensemble, offsets, observed, variances, whole, total, sums,
    own, notes, numbers, pieces, stage, all_notes, seen, picked, half, chunks, extras,
    twin, tables, anomalies, weighted, copied, send, recv, arrived, parted,
):
    x, y, z, c = here()
    size = own.shape[1] // (PLANE * SIDE_Z)
    members = sums.shape[1]
    seat = c * SIDE_X + x
    loads = [
        pltpu.make_async_copy(ensemble, own, copied.at[0]),
        pltpu.make_async_copy(offsets.at[0], numbers, copied.at[1]),
        pltpu.make_async_copy(observed.at[0], notes.at[pl.ds(1, 1), :], copied.at[2]),
        pltpu.make_async_copy(variances.at[0], notes.at[pl.ds(2, 1), :], copied.at[3]),
    ]
    for load in loads:
        load.start()
    barrier = pltpu.get_barrier_semaphore()
    greet(barrier)
    for load in loads:
        load.wait()
    notes[0:1, :] = numbers[...].astype(jnp.float32)
    count, watches = notes.shape[1], all_notes.shape[2]
    to = lax.broadcasted_iota(jnp.int32, (count, watches), 1)
    at = lax.broadcasted_iota(jnp.int32, (count, watches), 0) + z * count
    row = lax.broadcasted_iota(jnp.int32, (8, count), 0)
    placed = dot6(
        jnp.where(row < 3, notes[...], 0.0), jnp.where(to == at, 1.0, 0.0).astype(jnp.float32)
    )
    mine = all_notes.at[SIDE_Z]
    mine[...] = placed

    @pl.loop(0, SIDE_Z)
    def _(t):
        pieces[t, y, seat] = own[:, links_of(block_of(x, y, t, c), size)]

    met(barrier)

    @pl.loop(1, SIDE_Z)
    def _(i):
        remote(mine, all_notes.at[z], send.at[0], recv.at[0], line_peer(i)).start()

    @pl.loop(0, SIDE_Z)
    def _(k):
        t = lax.rem(z + along(k), SIDE_Z)

        @pl.loop(1, PLANE)
        def _(i):
            px, py, _, pc = plane_peer(i)
            remote(
                own.at[:, links_of(block_of(px, py, t, pc), size)],
                pieces.at[t, y, seat],
                send.at[1],
                arrived.at[t],
                (px, py, z, pc),
            ).start()

    all_notes[z] = placed
    no_matter(all_notes.at[pl.ds(0, SIDE_Z - 1)], send.at[0], recv.at[0]).wait()
    table = jnp.sum(all_notes[pl.ds(0, SIDE_Z)], axis=0)
    offset = table[0:1, :].astype(jnp.int32)
    tables[c] = table
    remote(tables.at[c], tables.at[c], send.at[9], recv.at[9], (x, y, z, 1 - c)).start()
    link = lax.broadcasted_iota(jnp.int32, (size, watches), 0)
    seen[...] = jnp.where(link == offset, 1.0, 0.0).astype(jnp.bfloat16)
    line = lax.broadcasted_iota(jnp.int32, (members // SIDE_Z, watches), 1) // count

    def pass_on(k, part):
        t = lax.rem(z + along(k), SIDE_Z)
        some = pl.ds(part * (SIDE_Y // 2), SIDE_Y // 2)
        remote(
            stage.at[t, some], whole.at[some, z], send.at[3], recv.at[3], (x, y, t, c)
        ).start()

    def pick(k, found):
        t = lax.rem(z + along(k), SIDE_Z)
        no_matter(
            own.at[:, pl.ds(0, (PLANE - 1) * size)], send.at[1], arrived.at[t]
        ).wait_recv()

        def lay(j, _):
            stage[t, j] = pieces[t, j].reshape(stage.shape[2:])
            return 0

        lax.fori_loop(0, SIDE_Y, lay, 0)
        rows = stage[t].reshape(members // SIDE_Z, size)
        values = jnp.dot(rows, seen[...], preferred_element_type=jnp.float32)

        @pl.when(jnp.logical_and(k >= 1, k <= EARLY + HALVES))
        def _():
            pass_on(k - 1, 0)

        @pl.when(jnp.logical_and(k >= 1, k <= EARLY))
        def _():
            pass_on(k - 1, 1)

        return jnp.where(line == t, values, found)

    found = lax.fori_loop(0, SIDE_Z, pick, jnp.zeros(line.shape, jnp.float32))
    mine = picked.at[SIDE_Z]
    mine[...] = found.astype(jnp.bfloat16).reshape(mine.shape)

    @pl.loop(1, SIDE_Z)
    def _(i):
        remote(mine, picked.at[z], send.at[2], recv.at[2], line_peer(i)).start()

    @pl.loop(EARLY, EARLY + HALVES)
    def _(k):
        pass_on(k, 1)

    @pl.loop(EARLY + HALVES, SIDE_Z - 1)
    def _(k):
        pass_on(k, 0)
        pass_on(k, 1)

    picked[z] = mine[...]
    whole[:, z] = stage[z]
    no_matter(
        own.at[:, pl.ds(0, (PLANE - 1) * SIDE_Z * size)], send.at[1], recv.at[1]
    ).wait_send()
    no_matter(picked.at[pl.ds(0, SIDE_Z - 1)], send.at[2], recv.at[2]).wait()

    partner = (x, y, z, 1 - c)
    near = picked.at[pl.ds(0, SIDE_Z)]
    remote(near, twin, send.at[4], recv.at[4], partner).start()

    def terms(found, facts, core):
        measured, variance = facts[1:2, :], facts[2:3, :]
        values = jnp.swapaxes(found, 0, 1).reshape(members, watches).astype(jnp.float32)
        center = jnp.sum(values, axis=0, keepdims=True) * (1.0 / members)
        anomaly = values - center
        innovation = measured - center
        weight = 1.0 / ((members - 1.0) * variance)
        at = links_of(core, watches)
        anomalies[:, at] = anomaly
        weighted[:, at] = anomaly * weight
        return anomaly, innovation, weight, variance

    anomaly, innovation, weight, variance = terms(picked[pl.ds(0, SIDE_Z)], table, c)
    spread = jnp.sum(anomaly * anomaly, axis=0, keepdims=True) * (1.0 / (members - 1.0)) + variance
    column = dot6_t(weight * innovation, anomaly)
    numer = jnp.sum(innovation * innovation, axis=1, keepdims=True)
    denom = jnp.sum(spread, axis=1, keepdims=True)
    lane = lax.broadcasted_iota(jnp.int32, column.shape, 1)
    extra = extras.at[PLANE]
    extra[0:1, :] = column
    extra[1:2, :] = jnp.where(lane == 0, numer, jnp.where(lane == 1, denom, 0.0))

    @pl.loop(1, PLANE)
    def _(i):
        remote(
            extra, extras.at[y * (CORES * SIDE_X) + seat], send.at[5], recv.at[5], plane_peer(i)
        ).start()

    extras[y * (CORES * SIDE_X) + seat] = extra[...]
    no_matter(tables.at[0], send.at[9], recv.at[9]).wait()
    no_matter(twin, send.at[4], recv.at[4]).wait()
    terms(twin[...], tables[1 - c], 1 - c)

    tiles = members // TILE
    blocks = [(i, j) for i in range(tiles) for j in range(i + 1)]
    rows = half.shape[0]
    count = rows // TILE
    for k in range(count):
        (i0, j0), (i1, j1) = blocks[k], blocks[count + k]
        i, j = jnp.where(c == 0, i0, i1), jnp.where(c == 0, j0, j1)
        half[k * TILE : (k + 1) * TILE, :] = dot6_t(
            weighted[links_of(i, TILE), :], anomalies[links_of(j, TILE), :]
        )

    chips = SIDE_X * SIDE_Y
    part = rows // chips

    def part_of(px, py):
        return pl.ds(pl.multiple_of((py * SIDE_X + px) * part, part), part)

    @pl.loop(1, chips)
    def _(i):
        place = chip_peer(i)
        remote(
            half.at[part_of(place[0], place[1])],
            chunks.at[y * SIDE_X + x],
            send.at[6],
            recv.at[6],
            place,
        ).start()

    chunks[y * SIDE_X + x] = half[part_of(x, y), :]
    no_matter(chunks.at[pl.ds(0, chips - 1)], send.at[6], recv.at[6]).wait()
    done = total.at[c, part_of(x, y)]
    done[...] = jnp.sum(chunks[...], axis=0)

    @pl.loop(1, chips)
    def _(i):
        place = chip_peer(i)
        remote(done, done, send.at[7], parted.at[y * SIDE_X + x], place).start()

    remote(done, done, send.at[8], recv.at[8], partner).start()

    @pl.loop(1, chips)
    def _(i):
        px, py, _, _ = chip_peer(chips - i)
        piece = total.at[c, part_of(px, py)]
        no_matter(piece, send.at[7], parted.at[py * SIDE_X + px]).wait_recv()
        remote(piece, piece, send.at[8], recv.at[8], partner).start()

    no_matter(half.at[pl.ds(0, rows - part)], send.at[7], recv.at[7]).wait_send()
    no_matter(extras.at[pl.ds(0, PLANE - 1)], send.at[5], recv.at[5]).wait()
    sums[...] = jnp.sum(extras[pl.ds(0, PLANE)], axis=0)
    no_matter(half, send.at[8], recv.at[8]).wait()
    no_matter(stage.at[pl.ds(0, SIDE_Z - 1)], send.at[3], recv.at[3]).wait()


def scatter_kernel(
    high, low, state, own, whole, far, near, send_far, arrived, send_near, recv_near,
    send_last, recv_last, send_own, recv_own,
):
    x, y, z, c = here()
    rows, size = state.shape
    chip, seat = x * SIDE_Y + y, c * SIDE_X + x
    cut = far.shape[-1]
    first, second = pl.ds(0, cut), pl.ds(cut, size - cut)
    barrier = pltpu.get_barrier_semaphore()
    greet(barrier)
    wide = 512


    def analyse(k):
        at = links_of(k, wide)
        values = dot1(high[...], state[:, at]) + dot1(low[...], state[:, at])
        whole[:, :, :, :, at] = values.astype(jnp.bfloat16).reshape(*whole.shape[:-1], wide)

    pl.loop(0, size // wide)(analyse)
    met(barrier)

    @pl.loop(0, SIDE_Z - 1)
    def _(k):
        t = lax.rem(z + along(k), SIDE_Z)

        @pl.loop(0, SIDE_Y)
        def _(dy):
            py = lax.rem(y + dy, SIDE_Y)
            remote(
                whole.at[py, t, :, :, first],
                far.at[z * SIDE_Y + py],
                send_far,
                arrived.at[z, py],
                (x, y, t, c),
            ).start()

    @pl.loop(1, PLANE)
    def _(i):
        px, py, _, pc = plane_peer(i)
        remote(
            whole.at[py, :, pc * SIDE_X + px, :, second],
            near.at[:, chip, c],
            send_near,
            recv_near,
            (px, py, z, pc),
        ).start()

    def hand_on(source, py, dy, t):
        @pl.loop(jnp.where(dy == 0, 1, 0), CORES * SIDE_X)
        def _(j):
            px = lax.rem(x + lax.rem(j, SIDE_X), SIDE_X)
            pc = lax.rem(c + j // SIDE_X, CORES)
            remote(
                source(pc * SIDE_X + px),
                own.at[chip, t, c, :, first],
                send_last,
                recv_last,
                (px, py, z, pc),
            ).start()

        @pl.when(dy == 0)
        def _():
            own[chip, t, c, :, first] = source(seat)[...]

    @pl.loop(0, SIDE_Y)
    def _(dy):
        py = lax.rem(y + dy, SIDE_Y)
        hand_on(lambda s: whole.at[py, z, s, :, first], py, dy, z)

    @pl.loop(0, SIDE_Z)
    def _(t):
        near[t, chip, c] = whole[y, t, seat, :, second]

    def take(k):
        t = lax.rem(z + SIDE_Z - along(k), SIDE_Z)

        @pl.loop(0, SIDE_Y)
        def _(dy):
            py = lax.rem(y + dy, SIDE_Y)
            no_matter(far.at[t * SIDE_Y + py], send_far, arrived.at[t, py]).wait_recv()
            hand_on(lambda s: far.at[t * SIDE_Y + py, s], py, dy, t)

    pl.loop(0, HALFWAY)(take)
    chips = SIDE_X * SIDE_Y
    others = far.at[pl.ds(0, PLANE - 1)]
    no_matter(others, send_near, recv_near).wait()

    @pl.loop(0, SIDE_Z - 1)
    def _(k):
        t = lax.rem(z + along(k), SIDE_Z)
        remote(
            near.at[t], own.at[:, z, :, :, second], send_own, recv_own, (x, y, t, c)
        ).start()

    @pl.loop(0, chips)
    def _(i):
        own[i, z, :, :, second] = near[z, i]

    pl.loop(HALFWAY, SIDE_Z - 1)(take)
    no_matter(far.at[pl.ds(0, (SIDE_Z - 1) * SIDE_Y)], send_far, recv_near).wait_send()
    no_matter(near.at[pl.ds(0, SIDE_Z - 1)], send_own, recv_own).wait()
    no_matter(others, send_last, recv_last).wait()


VMEM = pl.BlockSpec(memory_space=pltpu.VMEM)
ROOM = 24 << 20


def gathered(own, offsets, observed, variances):
    rows = own.shape[0]
    size = own.shape[1] // (PLANE * SIDE_Z)
    members = rows * PLANE * SIDE_Z
    seats = CORES * SIDE_X
    count = offsets.shape[-1]
    watches = SIDE_Z * count
    tiles = members // TILE
    packed = tiles * (tiles + 1) // 2 * TILE // CORES
    part = packed // (SIDE_X * SIDE_Y)
    f32, bf16 = jnp.float32, jnp.bfloat16
    return pl.pallas_call(
        gather_kernel,
        name="gather",
        out_shape=(
            jax.ShapeDtypeStruct((SIDE_Y, SIDE_Z, seats * rows, size), bf16),
            jax.ShapeDtypeStruct((CORES, packed, TILE), f32),
            jax.ShapeDtypeStruct((2, members), f32),
        ),
        in_specs=[pl.BlockSpec(memory_space=pltpu.HBM)] * 4,
        out_specs=(VMEM, VMEM, VMEM),
        scratch_shapes=[
            pltpu.VMEM(own.shape, bf16),
            pltpu.VMEM((8, count), f32),
            pltpu.VMEM((1, count), jnp.int32),
            pltpu.VMEM((SIDE_Z, SIDE_Y, seats, rows, size), bf16),
            pltpu.VMEM((SIDE_Z, SIDE_Y, seats * rows, size), bf16),
            pltpu.VMEM((SIDE_Z + 1, 8, watches), f32),
            pltpu.VMEM((size, watches), bf16),
            pltpu.VMEM((SIDE_Z + 1, SIDE_Y, seats * rows, watches), bf16),
            pltpu.VMEM((packed, TILE), f32),
            pltpu.VMEM((SIDE_X * SIDE_Y, part, TILE), f32),
            pltpu.VMEM((PLANE + 1, 2, members), f32),
            pltpu.VMEM((SIDE_Z, SIDE_Y, seats * rows, watches), bf16),
            pltpu.VMEM((CORES, 8, watches), f32),
            pltpu.VMEM((members, CORES * watches), f32),
            pltpu.VMEM((members, CORES * watches), f32),
            pltpu.SemaphoreType.DMA((4,)),
            pltpu.SemaphoreType.DMA((10,)),
            pltpu.SemaphoreType.DMA((10,)),
            pltpu.SemaphoreType.DMA((SIDE_Z,)),
            pltpu.SemaphoreType.DMA((SIDE_X * SIDE_Y,)),
        ],
        compiler_params=pltpu.CompilerParams(
            collective_id=0, has_side_effects=True, vmem_limit_bytes=ROOM
        ),
    )(*(pltpu.with_memory_space_constraint(a, pltpu.HBM) for a in (own, offsets, observed, variances)))


def scattered(high, low, state, own_rows):
    rows, size = state.shape
    cut = size // 2
    chips, seats = SIDE_X * SIDE_Y, CORES * SIDE_X
    return pl.pallas_call(
        scatter_kernel,
        name="scatter",
        out_shape=jax.ShapeDtypeStruct((chips, SIDE_Z, CORES, own_rows, size), state.dtype),
        in_specs=[VMEM, VMEM, VMEM],
        out_specs=VMEM,
        scratch_shapes=[
            pltpu.VMEM((SIDE_Y, SIDE_Z, seats, own_rows, size), state.dtype),
            pltpu.VMEM((PLANE, seats, own_rows, cut), state.dtype),
            pltpu.VMEM((SIDE_Z, chips, CORES, own_rows, size - cut), state.dtype),
            pltpu.SemaphoreType.DMA,
            pltpu.SemaphoreType.DMA((SIDE_Z, SIDE_Y)),
            pltpu.SemaphoreType.DMA,
            pltpu.SemaphoreType.DMA,
            pltpu.SemaphoreType.DMA,
            pltpu.SemaphoreType.DMA,
            pltpu.SemaphoreType.DMA,
            pltpu.SemaphoreType.DMA,
        ],
        compiler_params=pltpu.CompilerParams(
            collective_id=1, has_side_effects=True, vmem_limit_bytes=ROOM
        ),
    )(high, low, state)


def split_bf16(a):
    high = a.astype(jnp.bfloat16)
    return high, (a - high.astype(jnp.float32)).astype(jnp.bfloat16)


def dot1(a, b):
    return jnp.dot(
        a.astype(jnp.bfloat16), b.astype(jnp.bfloat16), preferred_element_type=jnp.float32
    )


def dot6(a, b):
    return jnp.dot(a, b, precision=lax.Precision.HIGHEST, preferred_element_type=jnp.float32)


WELL_CONDITIONED = 2000.0
ROUNDING = 1e-6


def by_rows(rows, body, init=None):
    def step(i, carry):
        return body(pl.ds(pl.multiple_of(i * TILE, TILE), TILE), carry)

    return lax.fori_loop(0, rows // TILE, step, init)


def largest_row(m):
    return jnp.max(jnp.sum(jnp.abs(m), axis=1))


def sum_of_squares(m):
    return jnp.sum(m * m)


def unit(rows, n):
    row = lax.broadcasted_iota(jnp.int32, (TILE, n), 0) + rows.start
    col = lax.broadcasted_iota(jnp.int32, (TILE, n), 1)
    return jnp.where(row == col, 1.0, 0.0).astype(jnp.float32)


EXTRA = 16


def residual_squares(left):
    return jnp.sum(jnp.sum(left * left, axis=0, keepdims=True))


def quick_inverse(x, system, r, parts, both):
    n = system.shape[1]
    rows = system.shape[0]

    def passes(lhs, rhs):
        return jnp.dot(lhs, rhs, preferred_element_type=jnp.float32)

    values = system[...]
    high = values.astype(jnp.bfloat16)
    parts[pl.ds(0, rows), :] = high
    parts[pl.ds(rows, rows), :] = (values - high.astype(jnp.float32)).astype(jnp.bfloat16)
    top = pl.ds(0, n)
    r[...] = passes(parts[top, :], parts[top, :])
    square = r[...].astype(jnp.bfloat16)
    fourth = jnp.max(jnp.sum(jnp.abs(passes(square, square)), axis=0, keepdims=True))
    bound = jnp.sqrt(jnp.sqrt(fourth * 1.05))
    a = 2.0 / (1.0 + bound)

    def first(rows, total):
        eye = unit(rows, n)
        s = system[rows, :] * a
        left = eye - 2.0 * s + (a * a) * r[rows, :]
        grown = a * (2.0 * eye - s)
        x[rows, :] = grown
        both[rows, :] = grown.astype(jnp.bfloat16)
        both[pl.ds(n + rows.start, TILE), :] = left.astype(jnp.bfloat16)
        return total + jnp.sum(left * left, axis=0, keepdims=True)

    total = by_rows(n, first, jnp.zeros((1, n), jnp.float32))

    def more(state):
        count, size = state
        return jnp.logical_and(count < 16, size > 0.01)

    def double(state):
        count, _ = state
        out = passes(both[...], both[pl.ds(n, n), :])
        grown = x[top, :] + out[:n]
        left = out[n:]
        x[top, :] = grown
        both[...] = jnp.concatenate([grown, left]).astype(jnp.bfloat16)
        return count + 1, residual_squares(left)

    lax.while_loop(more, double, (jnp.int32(0), jnp.sum(total)))

    def more_newton(state):
        count, size = state
        return jnp.logical_and(count < 8, size > ROUNDING)

    def newton(state):
        count, _ = state
        now = x[top, :]
        xh = now.astype(jnp.bfloat16)
        xl = (now - xh.astype(jnp.float32)).astype(jnp.bfloat16)
        here_high = parts[pl.ds(0, rows), :]
        out = passes(here_high, xh) + (
            passes(here_high, xl) + passes(parts[pl.ds(rows, rows), :], xh)
        )
        r[...] = out[:n]

        def left_of(at, total):
            left = unit(at, n) - r[at, :]
            both[at, :] = left.astype(jnp.bfloat16)
            return total + jnp.sum(left * left, axis=0, keepdims=True)

        total = by_rows(n, left_of, jnp.zeros((1, n), jnp.float32))
        tail = out[n:]
        grown = jnp.concatenate([now, tail])
        x[...] = grown + passes(jnp.concatenate([xh, tail.astype(jnp.bfloat16)]), both[top, :])
        return count + 1, jnp.sum(total)

    return lax.while_loop(more_newton, newton, (jnp.int32(0), jnp.float32(1.0)))[1]


def careful_inverse(x, system, r, tmp):
    n = system.shape[1]

    def square(rows, bound):
        tmp[rows, :] = dot6(system[rows, :], system[pl.ds(0, n), :])
        return jnp.maximum(bound, largest_row(tmp[rows, :]))

    bound = jnp.sqrt(by_rows(n, square, jnp.float32(0.0)) * 1.02)
    a = 2.0 / (1.0 + bound)

    def first(rows, total):
        eye = unit(rows, n)
        s = system[rows, :] * a
        x[rows, :] = a * (2.0 * eye - s)
        left = eye - 2.0 * s + (a * a) * tmp[rows, :]
        r[rows, :] = left
        return total + sum_of_squares(left)

    def more(state):
        count, size = state
        return jnp.logical_and(count < 40, size > 4e-4)

    def double(state):
        def grow(rows, _):
            x[rows, :] += dot6(x[rows, :], r[...])
            tmp[rows, :] = dot6(r[rows, :], r[...])
            return 0

        by_rows(n, grow, 0)

        def take(rows, total):
            left = tmp[rows, :]
            r[rows, :] = left
            return total + sum_of_squares(left)

        return state[0] + 1, by_rows(n, take, jnp.float32(0.0))

    lax.while_loop(more, double, (jnp.int32(0), by_rows(n, first, jnp.float32(0.0))))

    def more_newton(state):
        count, size = state
        return jnp.logical_and(count < 12, size > ROUNDING)

    def newton(state):
        def residual(rows, total):
            left = unit(rows, n) - dot6(system[rows, :], x[pl.ds(0, n), :])
            r[rows, :] = left
            return total + sum_of_squares(left)

        size = by_rows(n, residual, jnp.float32(0.0))

        def correct(rows, _):
            x[rows, :] += dot6(x[rows, :], r[...])
            return 0

        by_rows(n, correct, 0)
        return state[0] + 1, size

    lax.while_loop(more_newton, newton, (jnp.int32(0), jnp.float32(1.0)))
    last = pl.ds(n, system.shape[0] - n)
    x[last, :] = dot6(system[last, :], x[pl.ds(0, n), :])


def mixing_kernel(products, sums, high, low, x, system, r, parts, both):
    n = sums.shape[1]
    tiles = n // TILE
    square = jnp.sum(sums[1:2, 0:1] / sums[1:2, 1:2])
    inflation = jnp.sqrt(jnp.full((1, n), square, jnp.float32))
    row = lax.broadcasted_iota(jnp.int32, (TILE, TILE), 0)
    col = lax.broadcasted_iota(jnp.int32, (TILE, TILE), 1)
    eye = jnp.where(row == col, 1.0, 0.0).astype(jnp.float32)
    corners = [i * (i + 3) // 2 for i in range(tiles)]
    diagonal = sum(products[block] for block in corners)
    trace = jnp.sum(jnp.sum(eye * diagonal, axis=0, keepdims=True)) * square
    shift = trace / ((n - 1.0) * n)
    block = 0
    for i in range(tiles):
        down = pl.ds(i * TILE, TILE)
        for j in range(i + 1):
            across = pl.ds(j * TILE, TILE)
            values = products[block] * square + shift
            if i == j:
                system[down, down] = values + eye
            else:
                system[down, across] = values
                system[across, down] = values.T
            block += 1

    def longest(rows, most):
        return most + jnp.sum(jnp.abs(system[rows, :]), axis=0, keepdims=True)

    most = jnp.max(by_rows(n, longest, jnp.zeros((1, n), jnp.float32)))
    first = lax.broadcasted_iota(jnp.int32, (EXTRA, n), 0) == 0
    system[pl.ds(n, EXTRA), :] = jnp.where(first, sums[0:1, :], 0.0)
    left = lax.cond(
        most < WELL_CONDITIONED,
        lambda: quick_inverse(x, system, r, parts, both),
        lambda: jnp.float32(1.0),
    )

    @pl.when(jnp.logical_not(left <= ROUNDING))
    def _():
        pl.run_scoped(
            lambda tmp: careful_inverse(x, system, r, tmp), pltpu.VMEM((n, n), jnp.float32)
        )

    q = x[pl.ds(n, 1), :] * square

    def mix(rows, _):
        eye = unit(rows, n)
        mixing = (0.5 * inflation) * (eye + x[rows, :]) + q
        mean = jnp.sum(mixing, axis=1, keepdims=True) * (1.0 / n)
        high[rows, :], low[rows, :] = split_bf16(mixing - mean + 1.0 / n)
        return 0

    by_rows(n, mix, 0)


def mixed(products, sums):
    n = sums.shape[1]
    return pl.pallas_call(
        mixing_kernel,
        name="mixing",
        out_shape=[jax.ShapeDtypeStruct((n, n), jnp.bfloat16)] * 2,
        in_specs=[VMEM, VMEM],
        out_specs=[VMEM, VMEM],
        scratch_shapes=[
            pltpu.VMEM((n + EXTRA, n), jnp.float32),
            pltpu.VMEM((n + EXTRA, n), jnp.float32),
            pltpu.VMEM((n, n), jnp.float32),
            pltpu.VMEM((2 * (n + EXTRA), n), jnp.bfloat16),
            pltpu.VMEM((2 * n, n), jnp.bfloat16),
        ],
        compiler_params=pltpu.CompilerParams(vmem_limit_bytes=ROOM),
    )(products.reshape(-1, TILE, TILE), sums)


def put_out_kernel(own, out, laid, done):
    size = own.shape[2]
    share = own.shape[0] // PARTS

    def part(k):
        return links_of(k, share * size)

    @pl.loop(0, PARTS)
    def _(k):
        for i in range(share):
            laid[:, links_of(k * share + i, size)] = own[k * share + i]

        pltpu.make_async_copy(laid.at[:, part(k)], out.at[:, part(k)], done.at[k]).start()

    @pl.loop(0, PARTS)
    def _(k):
        pltpu.make_async_copy(laid.at[:, part(k)], out.at[:, part(k)], done.at[k]).wait()


PARTS = 8


def put_out(own):
    rows, size = own.shape[-2:]
    own = own.reshape(-1, rows, size)
    shape = (rows, len(own) * size)
    return pl.pallas_call(
        put_out_kernel,
        name="put_out",
        out_shape=jax.ShapeDtypeStruct(shape, own.dtype),
        in_specs=[VMEM],
        out_specs=pl.BlockSpec(memory_space=pltpu.HBM),
        scratch_shapes=[pltpu.VMEM(shape, own.dtype), pltpu.SemaphoreType.DMA((PARTS,))],
        compiler_params=pltpu.CompilerParams(vmem_limit_bytes=ROOM),
    )(own)


def local(ensemble, obs_offset, observed, obs_var):
    state, products, sums = gathered(ensemble, obs_offset, observed, obs_var)
    high, low = mixed(products, sums)
    return put_out(scattered(high, low, state.reshape(sums.shape[1], -1), len(ensemble)))


def solution(mesh):
    finer = Mesh(
        mesh.devices.reshape(4, 8, 2, mesh.shape["region"]),
        ("member_0", "member_1", "member_2", "region"),
    )
    in_specs = (
        P(MEMBER_REGION, None),
        P("region", MEMBER, None),
        P("region", MEMBER, None),
        P("region", MEMBER, None),
    )
    out_specs = P(MEMBER_REGION, None)
    return jax.shard_map(local, mesh=finer, in_specs=in_specs, out_specs=out_specs, check_vma=False)
```
